64 devices in a mesh: dp: 4 (over x, y), tp: 16 (over z, core).
Axes of the slice: x: 2, y: 2, z: 8, core: 2. Of those that a mesh axis runs over, the one named last changes fastest.
The devices are a block of a 4x4x8 slice.
Arguments:
- tokens_in: bfloat16 [128, 256, 1024], P('dp'), parts along dimension 0
- ln_scale: bfloat16 [2, 1024], replicated
- w_query: bfloat16 [2, 1024, 1024], P(None, None, 'tp')
- w_key: bfloat16 [2, 1024, 1024], P(None, None, 'tp')
- w_value: bfloat16 [2, 1024, 1024], P(None, None, 'tp')
- q_scale: bfloat16 [2, 64], replicated
- k_scale: bfloat16 [2, 64], replicated
- w_out: bfloat16 [2, 1024, 1024], P(None, 'tp')
- b_out: bfloat16 [2, 1024], replicated
- w_up: bfloat16 [2, 1024, 4096], P(None, None, 'tp')
- b_up: bfloat16 [2, 4096], P(None, 'tp')
- w_down: bfloat16 [2, 4096, 1024], P(None, 'tp')
- b_down: bfloat16 [2, 1024], replicated
Outputs:
- output: bfloat16 [128, 256, 1024], P('dp'), parts along dimension 0
There are 4 independent parts. The reference program is written for one: setup_inputs(seed, part) draws one part's arguments, and reference() takes and returns one part's arrays. A program takes and returns all parts, laid end to end along the dimension named above; an argument that names none is the same for every part.
All inputs are finite; a program needn't handle non-finite values.
Results may differ from the reference program's by a relative error of at most 0.0156837.
Values are sent between devices in bfloat16 or wider.
A program may use at most 768 MiB of HBM per device.

```python
import jax
import jax.numpy as jnp
from jax import lax

IMAGES = 32
SEQ_LEN = 256
MODEL_DIM = 1024
NUM_HEADS = 16
HEAD_DIM = 64
MLP_DIM = 4096
LAYERS = 2
LN_EPS = 1e-6


def setup_inputs(seed: int = 0, part: int = 0) -> dict:
    base_key = jax.random.key(seed)
    part_key = jax.random.fold_in(base_key, part)
    key_list = jax.random.split(base_key, 12)
    hidden = NUM_HEADS * HEAD_DIM

    def normal(rng_key, arr_shape, spread, offset):
        std_draw = jax.random.normal(rng_key, arr_shape, jnp.float32)
        return (offset + spread * std_draw).astype(jnp.bfloat16)

    return {
        "tokens_in": normal(part_key, (IMAGES, SEQ_LEN, MODEL_DIM), 1.0, 0.0),
        "ln_scale": normal(key_list[0], (LAYERS, MODEL_DIM), 0.3, 1.0),
        "w_query": normal(key_list[1], (LAYERS, MODEL_DIM, hidden), MODEL_DIM ** -0.5, 0.0),
        "w_key": normal(key_list[2], (LAYERS, MODEL_DIM, hidden), MODEL_DIM ** -0.5, 0.0),
        "w_value": normal(key_list[3], (LAYERS, MODEL_DIM, hidden), MODEL_DIM ** -0.5, 0.0),
        "q_scale": normal(key_list[4], (LAYERS, HEAD_DIM), 0.3, 1.5),
        "k_scale": normal(key_list[5], (LAYERS, HEAD_DIM), 0.3, 1.5),
        "w_out": normal(key_list[6], (LAYERS, hidden, MODEL_DIM), hidden ** -0.5, 0.0),
        "b_out": normal(key_list[7], (LAYERS, MODEL_DIM), 0.5, 0.0),
        "w_up": normal(key_list[8], (LAYERS, MODEL_DIM, MLP_DIM), MODEL_DIM ** -0.5, 0.0),
        "b_up": normal(key_list[9], (LAYERS, MLP_DIM), 0.5, 0.0),
        "w_down": normal(key_list[10], (LAYERS, MLP_DIM, MODEL_DIM), MLP_DIM ** -0.5, 0.0),
        "b_down": normal(key_list[11], (LAYERS, MODEL_DIM), 0.5, 0.0),
    }


def layer_norm(values, scale_vec):
    mean_val = jnp.mean(values, axis=-1, keepdims=True)
    centered = values - mean_val
    variance = jnp.mean(centered * centered, axis=-1, keepdims=True)
    return centered * lax.rsqrt(variance + LN_EPS) * scale_vec.astype(jnp.float32)


def one_layer(tokens_in, ln_scale, w_query, w_key, w_value, q_scale, k_scale, w_out, b_out, w_up, b_up, w_down, b_down):
    n_tokens = IMAGES * SEQ_LEN
    residual = tokens_in.reshape(n_tokens, MODEL_DIM).astype(jnp.float32)
    normed = layer_norm(residual, ln_scale).astype(jnp.bfloat16)

    def project(weight):
        projected = jnp.dot(normed, weight, preferred_element_type=jnp.float32)
        return projected.reshape(IMAGES, SEQ_LEN, NUM_HEADS, HEAD_DIM)

    queries = layer_norm(project(w_query), q_scale).astype(jnp.bfloat16)
    keys_all = layer_norm(project(w_key), k_scale).astype(jnp.bfloat16)
    values_all = project(w_value).astype(jnp.bfloat16)

    def attend(operands):
        q_img, k_img, v_img = operands
        scores = jnp.einsum("qhd,khd->hqk", q_img.astype(jnp.float32), k_img.astype(jnp.float32)) * HEAD_DIM ** -0.5
        attn_prob = jax.nn.softmax(scores, axis=-1).astype(jnp.bfloat16)
        mixed_val = jnp.einsum("hqk,khd->qhd", attn_prob.astype(jnp.float32), v_img.astype(jnp.float32))
        return mixed_val.astype(jnp.bfloat16)

    attended = lax.map(attend, (queries, keys_all, values_all)).reshape(n_tokens, NUM_HEADS * HEAD_DIM)
    attn_part = jnp.dot(attended, w_out, preferred_element_type=jnp.float32)
    pre_act = jnp.dot(normed, w_up, preferred_element_type=jnp.float32) + b_up.astype(jnp.float32)
    activated = jax.nn.gelu(pre_act, approximate=True).astype(jnp.bfloat16)
    mlp_part = jnp.dot(activated, w_down, preferred_element_type=jnp.float32)
    summed = residual + b_out.astype(jnp.float32) + b_down.astype(jnp.float32) + attn_part + mlp_part
    return summed.astype(jnp.bfloat16).reshape(IMAGES, SEQ_LEN, MODEL_DIM)


def reference(tokens_in, ln_scale, w_query, w_key, w_value, q_scale, k_scale, w_out, b_out, w_up, b_up, w_down, b_down):
    def step_fn(state_in, params):
        return one_layer(state_in, *params), None

    encoded, _ = lax.scan(step_fn, tokens_in, (ln_scale, w_query, w_key, w_value, q_scale, k_scale, w_out, b_out, w_up, b_up, w_down, b_down))
    return encoded
```

```python
import functools

import jax
import jax.numpy as jnp
from jax import lax
from jax.experimental import pallas as pl
from jax.experimental.pallas import tpu as pltpu
from jax.sharding import PartitionSpec as P

LN_EPS = 1e-6
LOG2E = 1.4426950408889634
VMEM_BYTES = 48 * 1024 * 1024


def norm_rows(values, scale_row):
    mean_val = jnp.mean(values, axis=-1, keepdims=True)
    centered = values - mean_val
    variance = jnp.mean(centered * centered, axis=-1, keepdims=True)
    return (centered * lax.rsqrt(variance + LN_EPS) * scale_row).astype(jnp.bfloat16)


def norm_cols(values, scale_col):
    mean_val = jnp.mean(values, axis=0, keepdims=True)
    centered = values - mean_val
    variance = jnp.mean(centered * centered, axis=0, keepdims=True)
    return (centered * lax.rsqrt(variance + LN_EPS) * scale_col).astype(jnp.bfloat16)


def branches(normed, w_ref, b_up, q_col, k_col, seq_len, head_dim):
    tokens = normed.shape[0]
    mlp = b_up.shape[1]
    qkv = 3 * head_dim
    up_end = qkv + mlp
    proj = lax.dot_general(w_ref[0:qkv], normed, (((1,), (1,)), ((), ())), preferred_element_type=jnp.float32)
    queries = norm_cols(proj[0:head_dim], q_col)
    keys_all = norm_cols(proj[head_dim : 2 * head_dim], k_col)
    values_all = proj[2 * head_dim : qkv].astype(jnp.bfloat16)
    pre_act = lax.dot_general(normed, w_ref[qkv:up_end], (((1,), (1,)), ((), ())), preferred_element_type=jnp.float32)
    activated = jax.nn.gelu(pre_act + b_up, approximate=True).astype(jnp.bfloat16)
    mixed = []
    for img in range(tokens // seq_len):
        cols = slice(img * seq_len, (img + 1) * seq_len)
        scores = lax.dot_general(keys_all[:, cols], queries[:, cols], (((0,), (0,)), ((), ())), preferred_element_type=jnp.float32)
        top = jnp.max(scores, axis=0, keepdims=True)
        expd = jnp.exp2((scores - top) * (LOG2E * head_dim**-0.5))
        prob = (expd * (1.0 / jnp.sum(expd, axis=0, keepdims=True))).astype(jnp.bfloat16)
        mixed.append(jnp.dot(values_all[:, cols], prob, preferred_element_type=jnp.float32))
    mixed_rows = jnp.concatenate(mixed, axis=1).T.astype(jnp.bfloat16)
    both = jnp.concatenate([activated, mixed_rows], axis=1)
    return jnp.dot(both, w_ref[up_end:], preferred_element_type=jnp.float32)


def first_kernel(seq_len, head_dim, x_ref, w_ref, ln_ref, b_ref, q_ref, k_ref, out_ref):
    normed = norm_rows(x_ref[...].astype(jnp.float32), ln_ref[...])
    out_ref[...] = branches(normed, w_ref, b_ref[...], q_ref[...], k_ref[...], seq_len, head_dim).astype(out_ref.dtype)


def second_kernel(seq_len, head_dim, x_ref, r_ref, bias0_ref, bias1_ref, w_ref, ln_ref, b_ref, q_ref, k_ref, out_ref, h_ref, acc_ref):
    step = pl.program_id(0)

    @pl.when(step == 0)
    def _():
        start = (x_ref[...].astype(jnp.float32) + bias0_ref[...] + r_ref[...].astype(jnp.float32)).astype(jnp.bfloat16).astype(jnp.float32)
        h_ref[...] = norm_rows(start, ln_ref[...])
        acc_ref[...] = start + bias1_ref[...]

    acc_ref[...] += branches(h_ref[...], w_ref.at[0], b_ref[0], q_ref[...], k_ref[...], seq_len, head_dim)

    @pl.when(step == pl.num_programs(0) - 1)
    def _():
        out_ref[...] = acc_ref[...].astype(out_ref.dtype)


def solution(mesh):
    col_spec = P(None, None, "tp")
    row_spec = P(None, "tp", None)
    in_specs = (P("dp", None, None), P(), col_spec, col_spec, col_spec, P(), P(), row_spec, P(), col_spec, P(None, "tp"), row_spec, P())
    tp = mesh.shape["tp"]
    dp = mesh.shape["dp"]

    def per_device(tokens_in, ln_scale, w_query, w_key, w_value, q_scale, k_scale, w_out, b_out, w_up, b_up, w_down, b_down):
        n_images, seq_len, model_dim = tokens_in.shape
        n_tokens = n_images * seq_len
        head_dim = q_scale.shape[1]
        mlp = w_up.shape[2]
        share = n_tokens // tp
        tokens = tokens_in.reshape(n_tokens, model_dim)
        f32 = jnp.float32

        def packed(layer):
            return jnp.concatenate([w_query[layer].T, w_key[layer].T, w_value[layer].T, w_up[layer].T, w_down[layer], w_out[layer]], axis=0)

        pack0, pack1 = packed(0), packed(1)
        rows = pack1.shape[0]
        piece = rows // dp
        mine = lax.dynamic_slice_in_dim(pack1, lax.axis_index("dp") * piece, piece, 0)
        gathered = lax.all_gather(mine, ("tp", "dp"), axis=0, tiled=True).reshape(tp, rows, model_dim)
        b_up_all = lax.all_gather(b_up[1:2].astype(f32), "tp", axis=0).reshape(tp, 1, mlp)
        bias = (b_out.astype(f32) + b_down.astype(f32)).reshape(-1, 1, model_dim)
        ln_rows = ln_scale.astype(f32).reshape(-1, 1, model_dim)
        q_cols = q_scale.astype(f32).reshape(-1, head_dim, 1)
        k_cols = k_scale.astype(f32).reshape(-1, head_dim, 1)

        def whole(shape):
            return pl.BlockSpec(shape, lambda i: (0,) * len(shape))

        flops = 2 * n_tokens * model_dim * (rows + seq_len // 2)
        part = pl.pallas_call(
            functools.partial(first_kernel, seq_len, head_dim),
            grid=(tp,),
            out_shape=jax.ShapeDtypeStruct((n_tokens, model_dim), jnp.bfloat16),
            in_specs=[
                pl.BlockSpec((share, model_dim), lambda i: (i, 0)),
                whole((rows, model_dim)), whole((1, model_dim)), whole((1, mlp)), whole((head_dim, 1)), whole((head_dim, 1)),
            ],
            out_specs=pl.BlockSpec((share, model_dim), lambda i: (i, 0)),
            compiler_params=pltpu.CompilerParams(vmem_limit_bytes=VMEM_BYTES),
            cost_estimate=pl.CostEstimate(flops=flops, bytes_accessed=4 * n_tokens * model_dim, transcendentals=0),
            name="first_layer",
        )(tokens, pack0, ln_rows[0], b_up[0:1].astype(f32), q_cols[0], k_cols[0])
        reduced = lax.psum_scatter(part, "tp", scatter_dimension=0, tiled=True)
        own = lax.dynamic_slice_in_dim(tokens, lax.axis_index("tp") * share, share, 0)
        out = pl.pallas_call(
            functools.partial(second_kernel, seq_len, head_dim),
            grid=(tp,),
            out_shape=jax.ShapeDtypeStruct((share, model_dim), jnp.bfloat16),
            in_specs=[
                whole((share, model_dim)), whole((share, model_dim)), whole((1, model_dim)), whole((1, model_dim)),
                pl.BlockSpec((1, rows, model_dim), lambda i: (i, 0, 0)),
                whole((1, model_dim)), pl.BlockSpec((1, 1, mlp), lambda i: (i, 0, 0)), whole((head_dim, 1)), whole((head_dim, 1)),
            ],
            out_specs=whole((share, model_dim)),
            scratch_shapes=[pltpu.VMEM((share, model_dim), jnp.bfloat16), pltpu.VMEM((share, model_dim), f32)],
            compiler_params=pltpu.CompilerParams(vmem_limit_bytes=VMEM_BYTES),
            cost_estimate=pl.CostEstimate(flops=flops, bytes_accessed=2 * tp * rows * model_dim, transcendentals=0),
            name="second_layer",
        )(own, reduced, bias[0], bias[1], gathered, ln_rows[1], b_up_all, q_cols[1], k_cols[1])
        encoded = lax.all_gather(out, "tp", axis=0, tiled=True)
        return encoded.reshape(n_images, seq_len, model_dim)

    return jax.shard_map(per_device, mesh=mesh, in_specs=in_specs, out_specs=P("dp", None, None), check_vma=False)
```

```python
import functools

import jax
import jax.numpy as jnp
from jax import lax
from jax.experimental import pallas as pl
from jax.experimental.pallas import tpu as pltpu
from jax.sharding import PartitionSpec as P

LN_EPS = 1e-6
LOG2E = 1.4426950408889634
VMEM_BYTES = 44 * 1024 * 1024
MESH = pl.DeviceIdType.MESH


def norm_rows(values, scale_row):
    mean_val = jnp.mean(values, axis=-1, keepdims=True)
    centered = values - mean_val
    variance = jnp.mean(centered * centered, axis=-1, keepdims=True)
    return (centered * lax.rsqrt(variance + LN_EPS) * scale_row).astype(jnp.bfloat16)


def norm_cols(values, scale_col):
    mean_val = jnp.mean(values, axis=0, keepdims=True)
    centered = values - mean_val
    variance = jnp.mean(centered * centered, axis=0, keepdims=True)
    return (centered * lax.rsqrt(variance + LN_EPS) * scale_col).astype(jnp.bfloat16)


def branches(normed, w_ref, b_up, q_col, k_col, seq_len, head_dim):
    tokens = normed.shape[0]
    mlp = b_up.shape[1]
    qkv = 3 * head_dim
    up_end = qkv + mlp
    proj = lax.dot_general(w_ref[0:qkv], normed, (((1,), (1,)), ((), ())), preferred_element_type=jnp.float32)
    queries = norm_cols(proj[0:head_dim], q_col)
    keys_all = norm_cols(proj[head_dim : 2 * head_dim], k_col)
    values_all = proj[2 * head_dim : qkv].astype(jnp.bfloat16)
    pre_act = lax.dot_general(normed, w_ref[qkv:up_end], (((1,), (1,)), ((), ())), preferred_element_type=jnp.float32)
    activated = jax.nn.gelu(pre_act + b_up, approximate=True).astype(jnp.bfloat16)
    mixed = []
    for img in range(tokens // seq_len):
        cols = slice(img * seq_len, (img + 1) * seq_len)
        scores = lax.dot_general(keys_all[:, cols], queries[:, cols], (((0,), (0,)), ((), ())), preferred_element_type=jnp.float32)
        top = jnp.max(scores, axis=0, keepdims=True)
        expd = jnp.exp2((scores - top) * (LOG2E * head_dim**-0.5))
        prob = (expd * (1.0 / jnp.sum(expd, axis=0, keepdims=True))).astype(jnp.bfloat16)
        mixed.append(jnp.dot(values_all[:, cols], prob, preferred_element_type=jnp.float32))
    mixed_rows = jnp.concatenate(mixed, axis=1).T.astype(jnp.bfloat16)
    both = jnp.concatenate([activated, mixed_rows], axis=1)
    return jnp.dot(both, w_ref[up_end:], preferred_element_type=jnp.float32)


def neighbours(tp):
    me = lax.axis_index("tp")
    chips = tp // 2
    core = lax.rem(me, 2)
    chip = me // 2
    right = lax.rem(chip + 1, chips) * 2 + core
    left = lax.rem(chip + chips - 1, chips) * 2 + core
    return core, chip, right, left, me + 1 - 2 * core


def enter(peers):
    barrier = pltpu.get_barrier_semaphore()
    for peer in peers:
        pl.semaphore_signal(barrier, inc=1, device_id={"tp": peer}, device_id_type=MESH)
    pl.semaphore_wait(barrier, len(peers))


def first_kernel(seq_len, head_dim, tp, x_hbm, w_ref, ln_ref, b_ref, q_ref, k_ref, bias_ref, y_ref, x_buf, ring, from_partner, to_partner, mine, x_sem, ring_send, ring_recv, pair_send, pair_recv):
    core, chip, right, left, partner = neighbours(tp)
    chips = tp // 2
    half = x_buf.shape[1] // 2
    sub_rows = half // 2
    items = 2 * chips
    enter((right, left, partner))

    def x_copies(item):
        way = lax.rem(item, 2)
        there = lax.rem(chip + 2 * chips + (1 + item // 2) * (2 * way - 1), chips)
        slot = lax.rem(item, 2)
        return [
            pltpu.make_async_copy(
                x_hbm.at[pl.ds(pl.multiple_of((2 * there + owner) * (2 * half) + way * half, half), half)],
                x_buf.at[slot, pl.ds(place * half, half)],
                x_sem.at[slot, place],
            )
            for place, owner in ((0, 1 - core), (1, core))
        ]

    def pair_copy(item):
        return pltpu.make_async_remote_copy(
            src_ref=to_partner.at[item], dst_ref=from_partner.at[item],
            send_sem=pair_send.at[item], recv_sem=pair_recv.at[item],
            device_id={"tp": partner}, device_id_type=MESH,
        )

    def ring_copy(step, way, sub):
        return pltpu.make_async_remote_copy(
            src_ref=ring.at[step, way, sub], dst_ref=ring.at[step + 1, way, sub],
            send_sem=ring_send.at[step, way, sub], recv_sem=ring_recv.at[step, way, sub],
            device_id={"tp": left if way else right}, device_id_type=MESH,
        )

    for copy in x_copies(0):
        copy.start()

    def turn(index, carry):
        t = index - 2

        @pl.when(t >= 0)
        def _():
            step = t // 2
            sub = lax.rem(t, 2)
            rows = pl.ds(pl.multiple_of(sub * sub_rows, sub_rows), sub_rows)
            for way in range(2):
                item = 2 * step + way

                @pl.when(sub == 0)
                def _():
                    pair_copy(item).wait_recv()

                local = from_partner[item, rows].astype(jnp.float32) + mine[lax.rem(item, 4), rows].astype(jnp.float32)

                @pl.when(step == 0)
                def _():
                    ring[0, way, sub] = local.astype(ring.dtype)

                @pl.when(step > 0)
                def _():
                    ring_copy(step - 1, way, sub).wait_recv()

                @pl.when(jnp.logical_and(step > 0, step < chips - 1))
                def _():
                    ring[step, way, sub] = (ring[step, way, sub].astype(jnp.float32) + local).astype(ring.dtype)

                @pl.when(step < chips - 1)
                def _():
                    ring_copy(step, way, sub).start()

                @pl.when(step == chips - 1)
                def _():
                    own = x_buf[way, pl.ds(pl.multiple_of(half + sub * sub_rows, sub_rows), sub_rows)].astype(jnp.float32)
                    total = ring[chips - 1, way, sub].astype(jnp.float32) + local
                    y_ref[pl.ds(pl.multiple_of(way * half + sub * sub_rows, sub_rows), sub_rows)] = (own + bias_ref[...] + total).astype(y_ref.dtype)

        @pl.when(index < items)
        def _():
            @pl.when(index + 1 < items)
            def _():
                for copy in x_copies(index + 1):
                    copy.start()

            for copy in x_copies(index):
                copy.wait()
            normed = norm_rows(x_buf[lax.rem(index, 2)].astype(jnp.float32), ln_ref[...])
            part = branches(normed, w_ref, b_ref[...], q_ref[...], k_ref[...], seq_len, head_dim).astype(jnp.bfloat16)
            to_partner[index] = part[:half]
            mine[lax.rem(index, 4)] = part[half:]
            pair_copy(index).start()

        return carry

    lax.fori_loop(0, items + 2, turn, 0)

    def drain(item, carry):
        pair_copy(item).wait_send()
        return carry

    lax.fori_loop(0, items, drain, 0)

    def drain_ring(step, carry):
        for way in range(2):
            for sub in range(2):
                ring_copy(step, way, sub).wait_send()
        return carry

    lax.fori_loop(0, chips - 1, drain_ring, 0)


def second_kernel(seq_len, head_dim, tp, dp, y_ref, w_hbm, ln_ref, bias_ref, q_ref, k_ref, out_ref, w_buf, h_ref, acc_ref, w_sem, ring_send, ring_recv, pair_send, pair_recv):
    core, chip, right, left, partner = neighbours(tp)
    chips = tp // 2
    share = y_ref.shape[0]
    images = share // seq_len
    rows = w_buf.shape[1] - 8
    piece = rows // dp
    sub_rows = seq_len // 4
    mlp = rows - 4 * head_dim - (rows - 4 * head_dim) // 2
    enter((right, left, partner))

    def w_copies(turn):
        shard = lax.rem(turn, tp)
        slot = lax.rem(turn, 2)
        copies = []
        for part in range(dp):
            base = (shard * dp + part) * (piece + 8)
            copies.append((pl.multiple_of(base, 8), piece, part * piece, part))
        copies.append((pl.multiple_of(shard * dp * (piece + 8) + piece, 8), 8, rows, dp))
        return [pltpu.make_async_copy(w_hbm.at[pl.ds(src, n)], w_buf.at[slot, pl.ds(dst, n)], w_sem.at[slot, place]) for src, n, dst, place in copies]

    def chunk(image, way, sub, owner):
        offset = owner * share + image * seq_len + way * (2 * sub_rows) + sub * sub_rows
        return out_ref.at[pl.ds(pl.multiple_of(offset, sub_rows), sub_rows)]

    def origin(way, step):
        back = chip - step if way == 0 else chip + step
        return 2 * lax.rem(back + chips, chips)

    def ring_copy(image, way, sub, step):
        ref = chunk(image, way, sub, origin(way, step) + core)
        return pltpu.make_async_remote_copy(
            src_ref=ref, dst_ref=ref, send_sem=ring_send.at[image, way, sub, step], recv_sem=ring_recv.at[image, way, sub, step],
            device_id={"tp": left if way else right}, device_id_type=MESH,
        )

    def arrival(image, way, sub, step):
        ref = chunk(image, way, sub, origin(way, step + 1) + core)
        return pltpu.make_async_remote_copy(
            src_ref=ref, dst_ref=ref, send_sem=ring_send.at[image, way, sub, step], recv_sem=ring_recv.at[image, way, sub, step],
            device_id={"tp": left if way else right}, device_id_type=MESH,
        )

    def pair_copy(image, way, sub, step, who):
        ref = chunk(image, way, sub, origin(way, step) + who)
        return pltpu.make_async_remote_copy(
            src_ref=ref, dst_ref=ref, send_sem=pair_send.at[image, way, sub, step], recv_sem=pair_recv.at[image, way, sub, step],
            device_id={"tp": partner}, device_id_type=MESH,
        )

    def event(image, number):
        step = number // 2
        sub = lax.rem(number, 2)
        for way in range(2):
            arrival(image, way, sub, step).wait_recv()

            @pl.when(step + 1 < chips - 1)
            def _():
                ring_copy(image, way, sub, step + 1).start()

            pair_copy(image, way, sub, step + 1, core).start()

    for copy in w_copies(0):
        copy.start()
    start = y_ref[...].astype(jnp.float32)
    h_ref[...] = norm_rows(start, ln_ref[...])
    acc_ref[...] = start + bias_ref[...]

    def turn(index, carry):
        image = index // tp
        shard = lax.rem(index, tp)

        @pl.when(index + 1 < images * tp)
        def _():
            for copy in w_copies(index + 1):
                copy.start()

        @pl.when(jnp.logical_and(image > 0, lax.rem(shard, 2) == 0))
        def _():
            event(image - 1, shard // 2)

        for copy in w_copies(index):
            copy.wait()
        slot = lax.rem(index, 2)
        span = pl.ds(pl.multiple_of(image * seq_len, seq_len), seq_len)
        b_up = w_buf[slot, pl.ds(rows, 8)].astype(jnp.float32)[0:1, 0:mlp]
        acc_ref[span] += branches(h_ref[span], w_buf.at[slot, pl.ds(0, rows)], b_up, q_ref[...], k_ref[...], seq_len, head_dim)

        @pl.when(shard == tp - 1)
        def _():
            me = 2 * chip + core
            out_ref[pl.ds(pl.multiple_of(me * share + image * seq_len, seq_len), seq_len)] = acc_ref[span].astype(out_ref.dtype)
            for sub in range(2):
                for way in range(2):
                    ring_copy(image, way, sub, 0).start()
            for sub in range(2):
                for way in range(2):
                    pair_copy(image, way, sub, 0, core).start()

        return carry

    lax.fori_loop(0, images * tp, turn, 0)
    total = 2 * (chips - 1)
    done = tp // 2

    def tail(number, carry):
        @pl.when(number + done < total)
        def _():
            event(images - 2, number + done)

        event(images - 1, number)
        return carry

    lax.fori_loop(0, total, tail, 0)

    def drain(step, carry):
        for image in range(images):
            for way in range(2):
                for sub in range(2):
                    @pl.when(step < chips - 1)
                    def _():
                        ring_copy(image, way, sub, step).wait_send()

                    pair_copy(image, way, sub, step, core).wait_send()
                    pair_copy(image, way, sub, step, 1 - core).wait_recv()
        return carry

    lax.fori_loop(0, chips, drain, 0)


def solution(mesh):
    col_spec = P(None, None, "tp")
    row_spec = P(None, "tp", None)
    in_specs = (P("dp", None, None), P(), col_spec, col_spec, col_spec, P(), P(), row_spec, P(), col_spec, P(None, "tp"), row_spec, P())
    tp = mesh.shape["tp"]
    dp = mesh.shape["dp"]
    chips = tp // 2

    def per_device(tokens_in, ln_scale, w_query, w_key, w_value, q_scale, k_scale, w_out, b_out, w_up, b_up, w_down, b_down):
        n_images, seq_len, model_dim = tokens_in.shape
        n_tokens = n_images * seq_len
        head_dim = q_scale.shape[1]
        mlp = w_up.shape[2]
        share = n_tokens // tp
        half = share // 2
        images = share // seq_len
        tokens = tokens_in.reshape(n_tokens, model_dim)
        f32, bf16 = jnp.float32, jnp.bfloat16

        def packed(layer):
            return jnp.concatenate([w_query[layer].T, w_key[layer].T, w_value[layer].T, w_up[layer].T, w_down[layer], w_out[layer]], axis=0)

        pack0, pack1 = packed(0), packed(1)
        rows = pack1.shape[0]
        piece = rows // dp
        bias_rows = jnp.pad(b_up[1:2], ((0, 7), (0, model_dim - mlp)))
        mine = jnp.concatenate([lax.dynamic_slice_in_dim(pack1, lax.axis_index("dp") * piece, piece, 0), bias_rows], axis=0)
        pack0, mine = lax.optimization_barrier((pack0, mine))
        gathered = lax.all_gather(mine, ("tp", "dp"), axis=0, tiled=True)
        bias = (b_out.astype(f32) + b_down.astype(f32)).reshape(-1, 1, model_dim)
        ln_rows = ln_scale.astype(f32).reshape(-1, 1, model_dim)
        q_cols = q_scale.astype(f32).reshape(-1, head_dim, 1)
        k_cols = k_scale.astype(f32).reshape(-1, head_dim, 1)
        vmem = pl.BlockSpec(memory_space=pltpu.VMEM)
        hbm = pl.BlockSpec(memory_space=pl.ANY)
        dma = pltpu.SemaphoreType.DMA
        flops = 2 * n_tokens * model_dim * (rows + seq_len // 2)
        middle = pl.pallas_call(
            functools.partial(first_kernel, seq_len, head_dim, tp),
            out_shape=jax.ShapeDtypeStruct((share, model_dim), bf16),
            in_specs=[hbm] + [vmem] * 6,
            out_specs=vmem,
            scratch_shapes=[
                pltpu.VMEM((2, share, model_dim), bf16),
                pltpu.VMEM((chips, 2, 2, half // 2, model_dim), bf16),
                pltpu.VMEM((tp, half, model_dim), bf16),
                pltpu.VMEM((tp, half, model_dim), bf16),
                pltpu.VMEM((4, half, model_dim), bf16),
                dma((2, 2)), dma((chips - 1, 2, 2)), dma((chips - 1, 2, 2)), dma((tp,)), dma((tp,)),
            ],
            compiler_params=pltpu.CompilerParams(vmem_limit_bytes=VMEM_BYTES, collective_id=0, has_side_effects=True),
            cost_estimate=pl.CostEstimate(flops=4 * flops, bytes_accessed=4 * n_tokens * model_dim, transcendentals=0),
            name="first_layer",
        )(tokens, pack0, ln_rows[0], b_up[0:1].astype(f32), q_cols[0], k_cols[0], bias[0])
        out = pl.pallas_call(
            functools.partial(second_kernel, seq_len, head_dim, tp, dp),
            out_shape=jax.ShapeDtypeStruct((n_tokens, model_dim), bf16),
            in_specs=[vmem, hbm] + [vmem] * 4,
            out_specs=vmem,
            scratch_shapes=[
                pltpu.VMEM((2, rows + 8, model_dim), bf16),
                pltpu.VMEM((share, model_dim), bf16), pltpu.VMEM((share, model_dim), f32),
                dma((2, dp + 1)), dma((images, 2, 2, chips)), dma((images, 2, 2, chips)), dma((images, 2, 2, chips)), dma((images, 2, 2, chips)),
            ],
            compiler_params=pltpu.CompilerParams(vmem_limit_bytes=VMEM_BYTES, collective_id=1, has_side_effects=True),
            cost_estimate=pl.CostEstimate(flops=4 * flops, bytes_accessed=2 * tp * rows * model_dim, transcendentals=0),
            name="second_layer",
        )(middle, gathered, ln_rows[1], bias[1], q_cols[1], k_cols[1])
        return out.reshape(n_images, seq_len, model_dim)

    return jax.shard_map(per_device, mesh=mesh, in_specs=in_specs, out_specs=P("dp", None, None), check_vma=False)
```

```python
import functools
import math

import jax
import jax.numpy as jnp
from jax import lax
from jax.experimental import pallas as pl
from jax.experimental.pallas import tpu as pltpu
from jax.sharding import PartitionSpec as P

LN_EPS = 1e-6
LOG2E = 1.4426950408889634
FIRST_VMEM = 46 * 1024 * 1024
SECOND_VMEM = 24 * 1024 * 1024
MESH = pl.DeviceIdType.MESH


def norm_rows(values, scale_row):
    mean_val = jnp.mean(values, axis=-1, keepdims=True)
    centered = values - mean_val
    variance = jnp.mean(centered * centered, axis=-1, keepdims=True)
    return (centered * lax.rsqrt(variance + LN_EPS) * scale_row).astype(jnp.bfloat16)


def norm_cols(values, scale_col):
    mean_val = jnp.mean(values, axis=0, keepdims=True)
    centered = values - mean_val
    variance = jnp.mean(centered * centered, axis=0, keepdims=True)
    return (centered * lax.rsqrt(variance + LN_EPS) * scale_col).astype(jnp.bfloat16)


def branches(normed, w_ref, b_up, q_col, k_col, seq_len, head_dim):
    tokens = normed.shape[0]
    mlp = b_up.shape[1]
    qkv = 3 * head_dim
    up_end = qkv + mlp
    proj = lax.dot_general(w_ref[0:qkv], normed, (((1,), (1,)), ((), ())), preferred_element_type=jnp.float32)
    queries = norm_cols(proj[0:head_dim], q_col)
    keys_all = norm_cols(proj[head_dim : 2 * head_dim], k_col)
    values_all = proj[2 * head_dim : qkv].astype(jnp.bfloat16)
    pre_act = lax.dot_general(normed, w_ref[qkv:up_end], (((1,), (1,)), ((), ())), preferred_element_type=jnp.float32)
    activated = jax.nn.gelu(pre_act + b_up, approximate=True).astype(jnp.bfloat16)
    mixed = []
    for img in range(tokens // seq_len):
        cols = slice(img * seq_len, (img + 1) * seq_len)
        scores = lax.dot_general(keys_all[:, cols], queries[:, cols], (((0,), (0,)), ((), ())), preferred_element_type=jnp.float32)
        top = jnp.max(scores, axis=0, keepdims=True)
        expd = jnp.exp2((scores - top) * (LOG2E * head_dim**-0.5))
        prob = (expd * (1.0 / jnp.sum(expd, axis=0, keepdims=True))).astype(jnp.bfloat16)
        mixed.append(jnp.dot(values_all[:, cols], prob, preferred_element_type=jnp.float32))
    mixed_rows = jnp.concatenate(mixed, axis=1).T.astype(jnp.bfloat16)
    both = jnp.concatenate([activated, mixed_rows], axis=1)
    return jnp.dot(both, w_ref[up_end:], preferred_element_type=jnp.float32)


def neighbours(tp):
    me = lax.axis_index("tp")
    chips = tp // 2
    core = lax.rem(me, 2)
    chip = me // 2
    right = lax.rem(chip + 1, chips) * 2 + core
    left = lax.rem(chip + chips - 1, chips) * 2 + core
    return core, chip, right, left, me + 1 - 2 * core


def enter(peers):
    barrier = pltpu.get_barrier_semaphore()
    for axis, peer in peers:
        pl.semaphore_signal(barrier, inc=1, device_id={axis: peer}, device_id_type=MESH)
    pl.semaphore_wait(barrier, len(peers))


def plane_of(dp):
    side = math.isqrt(dp)
    return (side, side) if side * side == dp else (1, dp)


def shard_of_round(chip, chips, number):
    sign = 1 - 2 * (number % 2)
    return lax.rem(chip + chips + sign * ((number + 1) // 2), chips)


def schedule_of(chips, plane):
    events = {}
    for number in range(chips):
        if number == 0:
            events[0] = [("pass", 0, 0), ("pair", 0, 0)]
            continue
        begin = max(3, 2 * number)
        events.setdefault(begin, []).append(("pass", number, 0))
        for hop in range(1, max(plane)):
            events.setdefault(begin + 1 + hop, []).append(("line", number, hop))
        for hop in range(1, max(plane)):
            events.setdefault(begin + 1 + max(plane) + hop, []).append(("plane", number, hop))
        events.setdefault(begin + 2 * max(plane), []).append(("pair", number, 0))
    return events


def first_kernel(seq_len, head_dim, tp, dp, x_hbm, wq_hbm, wk_hbm, wv_hbm, wup_hbm, wdown_hbm, wout_hbm, ln_ref, b_ref, q_ref, k_ref, bo_ref, bd_ref, y_ref, w_all, b_all, pack, up_raw, x_buf, ring, from_partner, to_partner, mine, load_sem, own_sem, x_sem, ring_send, ring_recv, pair_send, pair_recv, z_send, z_recv, zb_send, zb_recv, line_send, line_recv, plane_send, plane_recv, w_send, w_recv, wb_send, wb_recv):
    core, chip, right, left, partner = neighbours(tp)
    chips = tp // 2
    me = 2 * chip + core
    rows = pack.shape[1]
    mlp = up_raw.shape[2]
    qkv = 3 * head_dim
    plane = plane_of(dp)
    group = lax.axis_index("dp")
    at = (group // plane[1], lax.rem(group, plane[1]))
    unit = rows // (2 * dp)

    def group_at(axis, pos, other):
        return pos * plane[1] + other if axis == 0 else other * plane[1] + pos

    def beside(axis, sign):
        return group_at(axis, lax.rem(at[axis] + plane[axis] + sign, plane[axis]), at[1 - axis])

    half = x_buf.shape[1] // 2
    sub_rows = half // 2
    items = 2 * chips
    peers = [("tp", right), ("tp", left), ("tp", partner)]
    for axis in range(2):
        peers += [("dp", beside(axis, sign)) for sign in (1, -1)[: min(plane[axis] - 1, 2)]]
    enter(peers)

    def loads(layer):
        pieces = [(wq_hbm, pack.at[layer, 0:head_dim]), (wk_hbm, pack.at[layer, head_dim : 2 * head_dim]), (wv_hbm, pack.at[layer, 2 * head_dim : qkv]), (wup_hbm, up_raw.at[layer]), (wdown_hbm, pack.at[layer, qkv + mlp : qkv + 2 * mlp]), (wout_hbm, pack.at[layer, qkv + 2 * mlp : rows])]
        return [pltpu.make_async_copy(src.at[layer], dst, load_sem.at[layer, place]) for place, (src, dst) in enumerate(pieces)]

    def turn_up(layer):
        for copy in loads(layer):
            copy.wait()
        pack[layer, qkv : qkv + mlp] = up_raw[layer].T

    def block(number, start, count, owner):
        base = (2 * shard_of_round(chip, chips, number) + owner) * rows + start
        return w_all.at[pl.ds(pl.multiple_of(base, 8), count)]

    def z_copies(number):
        copies = []
        for part in range(2):
            rightwards = (part == 0) if number == chips - 1 else number % 2 == 1
            hops = (number + 1) // 2
            source = lax.rem(chip + chips + (1 - hops if rightwards else hops - 1), chips)
            peer = right if rightwards else left
            ref = w_all.at[pl.ds(pl.multiple_of((2 * source + core) * rows + (part * dp + group) * unit, 8), unit)]
            copies.append(pltpu.make_async_remote_copy(src_ref=ref, dst_ref=ref, send_sem=z_send.at[number, part], recv_sem=z_recv.at[number, part], device_id={"tp": peer}, device_id_type=MESH))
            if part == 0:
                ref = b_all.at[2 * source + core]
                copies.append(pltpu.make_async_remote_copy(src_ref=ref, dst_ref=ref, send_sem=zb_send.at[number], recv_sem=zb_recv.at[number], device_id={"tp": peer}, device_id_type=MESH))
        return copies

    def z_onward(number):
        if number == 0:
            return [(later, (0, 1)) for later in (1, 2) if later < chips - 1] or [(chips - 1, (0, 1))]
        if number + 2 < chips - 1:
            return [(number + 2, (0, 1))]
        if number < chips - 1:
            return [(chips - 1, (number % 2 == 0,))]
        return []

    def z_start(later, parts):
        copies = z_copies(later)
        for part in parts:
            if part == 0:
                copies[0].start()
                copies[1].start()
            else:
                copies[2].start()

    def axes(part):
        return (0, 1) if part == 0 else (1, 0)

    def sign_of(number):
        return 1 - 2 * (number % 2)

    def line_copy(number, part, hop):
        axis, sign = axes(part)[0], sign_of(number)
        source = group_at(axis, lax.rem(at[axis] + plane[axis] - sign * hop, plane[axis]), at[1 - axis])
        ref = block(number, (part * dp + source) * unit, unit, core)
        return pltpu.make_async_remote_copy(src_ref=ref, dst_ref=ref, send_sem=line_send.at[number, part, hop], recv_sem=line_recv.at[number, part, hop], device_id={"dp": beside(axis, sign)}, device_id_type=MESH)

    def plane_copy(number, part, off, hop):
        (one, two), sign = axes(part), sign_of(number)
        source = group_at(one, lax.rem(at[one] + plane[one] - sign * off, plane[one]), lax.rem(at[two] + plane[two] - sign * hop, plane[two]))
        ref = block(number, (part * dp + source) * unit, unit, core)
        return pltpu.make_async_remote_copy(src_ref=ref, dst_ref=ref, send_sem=plane_send.at[number, part, off, hop], recv_sem=plane_recv.at[number, part, off, hop], device_id={"dp": beside(two, sign)}, device_id_type=MESH)

    def w_pair(number, who):
        ref = block(number, 0, rows, who)
        bias = b_all.at[2 * shard_of_round(chip, chips, number) + who]
        return [
            pltpu.make_async_remote_copy(src_ref=ref, dst_ref=ref, send_sem=w_send.at[number], recv_sem=w_recv.at[number], device_id={"tp": partner}, device_id_type=MESH),
            pltpu.make_async_remote_copy(src_ref=bias, dst_ref=bias, send_sem=wb_send.at[number], recv_sem=wb_recv.at[number], device_id={"tp": partner}, device_id_type=MESH),
        ]

    def gather(kind, number, hop):
        if kind == "pass":
            if number > 0:
                for copy in z_copies(number):
                    copy.wait_recv()
            for later, parts in z_onward(number):
                z_start(later, parts)
            for part in range(2):
                if number > 0 and plane[axes(part)[0]] > 1:
                    line_copy(number, part, 0).start()
            for part in range(2):
                if number > 0 and plane[axes(part)[1]] > 1:
                    plane_copy(number, part, 0, 0).start()
        for part in range(2):
            one, two = (plane[axis] for axis in axes(part))
            if kind == "line" and hop < one:
                line_copy(number, part, hop - 1).wait_recv()
                if hop < one - 1:
                    line_copy(number, part, hop).start()
                if two > 1:
                    plane_copy(number, part, hop, 0).start()
            if kind == "plane" and hop < two:
                for off in range(one):
                    plane_copy(number, part, off, hop - 1).wait_recv()
                    if hop < two - 1:
                        plane_copy(number, part, off, hop).start()
        if kind == "pair":
            for copy in w_pair(number, core):
                copy.start()

    def x_copies(item):
        way = lax.rem(item, 2)
        there = lax.rem(chip + 2 * chips + (1 + item // 2) * (2 * way - 1), chips)
        slot = lax.rem(item, 2)
        return [
            pltpu.make_async_copy(
                x_hbm.at[pl.ds(pl.multiple_of((2 * there + owner) * (2 * half) + way * half, half), half)],
                x_buf.at[slot, pl.ds(place * half, half)],
                x_sem.at[slot, place],
            )
            for place, owner in ((0, 1 - core), (1, core))
        ]

    def pair_copy(item):
        return pltpu.make_async_remote_copy(
            src_ref=to_partner.at[item], dst_ref=from_partner.at[item],
            send_sem=pair_send.at[item], recv_sem=pair_recv.at[item],
            device_id={"tp": partner}, device_id_type=MESH,
        )

    def ring_copy(step, way, sub):
        return pltpu.make_async_remote_copy(
            src_ref=ring.at[step, way, sub], dst_ref=ring.at[step + 1, way, sub],
            send_sem=ring_send.at[step, way, sub], recv_sem=ring_recv.at[step, way, sub],
            device_id={"tp": left if way else right}, device_id_type=MESH,
        )

    for layer in (1, 0):
        for copy in loads(layer):
            copy.start()
    for copy in x_copies(0):
        copy.start()
    b_all[me] = jnp.broadcast_to(b_ref[1:2].astype(jnp.float32), b_all.shape[1:])
    turn_up(1)
    own_copy = pltpu.make_async_copy(pack.at[1], w_all.at[pl.ds(pl.multiple_of(me * rows, 8), rows)], own_sem)
    own_copy.start()
    turn_up(0)
    own_copy.wait()
    events = schedule_of(chips, plane)
    ln_row = ln_ref[0:1].astype(jnp.float32)
    b_row = b_ref[0:1].astype(jnp.float32)
    bias_row = bo_ref[0:1].astype(jnp.float32) + bd_ref[0:1].astype(jnp.float32)

    def turn(index, carry):
        t = index - 2

        @pl.when(t >= 0)
        def _():
            step = t // 2
            sub = lax.rem(t, 2)
            rows = pl.ds(pl.multiple_of(sub * sub_rows, sub_rows), sub_rows)
            for way in range(2):
                item = 2 * step + way

                @pl.when(sub == 0)
                def _():
                    pair_copy(item).wait_recv()

                local = from_partner[item, rows].astype(jnp.float32) + mine[lax.rem(item, 4), rows].astype(jnp.float32)

                @pl.when(step == 0)
                def _():
                    ring[0, way, sub] = local.astype(ring.dtype)

                @pl.when(step > 0)
                def _():
                    ring_copy(step - 1, way, sub).wait_recv()

                @pl.when(jnp.logical_and(step > 0, step < chips - 1))
                def _():
                    ring[step, way, sub] = (ring[step, way, sub].astype(jnp.float32) + local).astype(ring.dtype)

                @pl.when(step < chips - 1)
                def _():
                    ring_copy(step, way, sub).start()

                @pl.when(step == chips - 1)
                def _():
                    own = x_buf[way, pl.ds(pl.multiple_of(half + sub * sub_rows, sub_rows), sub_rows)].astype(jnp.float32)
                    total = ring[chips - 1, way, sub].astype(jnp.float32) + local
                    y_ref[pl.ds(pl.multiple_of(way * half + sub * sub_rows, sub_rows), sub_rows)] = (own + bias_row + total).astype(y_ref.dtype)

        for due, group_events in sorted(events.items()):
            if due < items + 2:
                @pl.when(index == due)
                def _():
                    for event in group_events:
                        gather(*event)

        @pl.when(index < items)
        def _():
            @pl.when(index + 1 < items)
            def _():
                for copy in x_copies(index + 1):
                    copy.start()

            for copy in x_copies(index):
                copy.wait()
            normed = norm_rows(x_buf[lax.rem(index, 2)].astype(jnp.float32), ln_row)
            part = branches(normed, pack.at[0], b_row, q_ref[0], k_ref[0], seq_len, head_dim).astype(jnp.bfloat16)
            to_partner[index] = part[:half]
            mine[lax.rem(index, 4)] = part[half:]
            pair_copy(index).start()

        return carry

    lax.fori_loop(0, items + 2, turn, 0)
    for due, group_events in sorted(events.items()):
        if due >= items + 2:
            for event in group_events:
                gather(*event)
    for number in range(chips):
        for copy in w_pair(number, core):
            copy.wait_send()
        for copy in w_pair(number, 1 - core):
            copy.wait_recv()
        for part in range(2 if number > 0 else 0):
            one, two = (plane[axis] for axis in axes(part))
            for hop in range(one - 1):
                line_copy(number, part, hop).wait_send()
            for hop in range(two - 1):
                for off in range(one):
                    plane_copy(number, part, off, hop).wait_send()
        if number > 0:
            for copy in z_copies(number):
                copy.wait_send()

    def drain(item, carry):
        pair_copy(item).wait_send()
        return carry

    lax.fori_loop(0, items, drain, 0)

    def drain_ring(step, carry):
        for way in range(2):
            for sub in range(2):
                ring_copy(step, way, sub).wait_send()
        return carry

    lax.fori_loop(0, chips - 1, drain_ring, 0)


def second_kernel(seq_len, head_dim, tp, y_ref, w_hbm, b_all, ln_ref, bo_ref, bd_ref, q_ref, k_ref, out_ref, w_buf, h_ref, acc_ref, w_sem, ring_send, ring_recv, pair_send, pair_recv):
    core, chip, right, left, partner = neighbours(tp)
    chips = tp // 2
    share = y_ref.shape[0]
    images = share // seq_len
    rows = w_buf.shape[1]
    sub_rows = seq_len // 4
    enter((("tp", right), ("tp", left), ("tp", partner)))

    def w_copy(turn):
        slot = lax.rem(turn, 2)
        return pltpu.make_async_copy(w_hbm.at[pl.ds(pl.multiple_of(lax.rem(turn, tp) * rows, 8), rows)], w_buf.at[slot], w_sem.at[slot])

    def chunk(image, way, sub, owner):
        offset = owner * share + image * seq_len + way * (2 * sub_rows) + sub * sub_rows
        return out_ref.at[pl.ds(pl.multiple_of(offset, sub_rows), sub_rows)]

    def origin(way, step):
        back = chip - step if way == 0 else chip + step
        return 2 * lax.rem(back + chips, chips)

    def ring_copy(image, way, sub, step):
        ref = chunk(image, way, sub, origin(way, step) + core)
        return pltpu.make_async_remote_copy(
            src_ref=ref, dst_ref=ref, send_sem=ring_send.at[image, way, sub, step], recv_sem=ring_recv.at[image, way, sub, step],
            device_id={"tp": left if way else right}, device_id_type=MESH,
        )

    def arrival(image, way, sub, step):
        ref = chunk(image, way, sub, origin(way, step + 1) + core)
        return pltpu.make_async_remote_copy(
            src_ref=ref, dst_ref=ref, send_sem=ring_send.at[image, way, sub, step], recv_sem=ring_recv.at[image, way, sub, step],
            device_id={"tp": left if way else right}, device_id_type=MESH,
        )

    def pair_copy(image, way, sub, step, who):
        ref = chunk(image, way, sub, origin(way, step) + who)
        return pltpu.make_async_remote_copy(
            src_ref=ref, dst_ref=ref, send_sem=pair_send.at[image, way, sub, step], recv_sem=pair_recv.at[image, way, sub, step],
            device_id={"tp": partner}, device_id_type=MESH,
        )

    def event(image, number):
        step = number // 2
        sub = lax.rem(number, 2)
        for way in range(2):
            arrival(image, way, sub, step).wait_recv()

            @pl.when(step + 1 < chips - 1)
            def _():
                ring_copy(image, way, sub, step + 1).start()

            pair_copy(image, way, sub, step + 1, core).start()

    w_copy(0).start()
    start = y_ref[...].astype(jnp.float32)
    h_ref[...] = norm_rows(start, ln_ref[1:2].astype(jnp.float32))
    acc_ref[...] = start + (bo_ref[1:2].astype(jnp.float32) + bd_ref[1:2].astype(jnp.float32))

    def turn(index, carry):
        image = index // tp
        shard = lax.rem(index, tp)

        @pl.when(index + 1 < images * tp)
        def _():
            w_copy(index + 1).start()

        @pl.when(jnp.logical_and(image > 0, lax.rem(shard, 2) == 0))
        def _():
            event(image - 1, shard // 2)

        w_copy(index).wait()
        slot = lax.rem(index, 2)
        span = pl.ds(pl.multiple_of(image * seq_len, seq_len), seq_len)
        acc_ref[span] += branches(h_ref[span], w_buf.at[slot], b_all[shard][0:1], q_ref[1], k_ref[1], seq_len, head_dim)

        @pl.when(shard == tp - 1)
        def _():
            me = 2 * chip + core
            out_ref[pl.ds(pl.multiple_of(me * share + image * seq_len, seq_len), seq_len)] = acc_ref[span].astype(out_ref.dtype)
            for sub in range(2):
                for way in range(2):
                    ring_copy(image, way, sub, 0).start()
            for sub in range(2):
                for way in range(2):
                    pair_copy(image, way, sub, 0, core).start()

        return carry

    lax.fori_loop(0, images * tp, turn, 0)
    total = 2 * (chips - 1)
    done = tp // 2

    def tail(number, carry):
        @pl.when(number + done < total)
        def _():
            event(images - 2, number + done)

        event(images - 1, number)
        return carry

    lax.fori_loop(0, total, tail, 0)

    def drain(step, carry):
        for image in range(images):
            for way in range(2):
                for sub in range(2):
                    @pl.when(step < chips - 1)
                    def _():
                        ring_copy(image, way, sub, step).wait_send()

                    pair_copy(image, way, sub, step, core).wait_send()
                    pair_copy(image, way, sub, step, 1 - core).wait_recv()
        return carry

    lax.fori_loop(0, chips, drain, 0)


def solution(mesh):
    col_spec = P(None, None, "tp")
    row_spec = P(None, "tp", None)
    in_specs = (P("dp", None, None), P(), col_spec, col_spec, col_spec, P(), P(), row_spec, P(), col_spec, P(None, "tp"), row_spec, P())
    tp = mesh.shape["tp"]
    dp = mesh.shape["dp"]
    chips = tp // 2

    def per_device(tokens_in, ln_scale, w_query, w_key, w_value, q_scale, k_scale, w_out, b_out, w_up, b_up, w_down, b_down):
        n_images, seq_len, model_dim = tokens_in.shape
        n_tokens = n_images * seq_len
        head_dim = q_scale.shape[1]
        mlp = w_up.shape[2]
        share = n_tokens // tp
        half = share // 2
        images = share // seq_len
        tokens = tokens_in.reshape(n_tokens, model_dim)
        f32, bf16 = jnp.float32, jnp.bfloat16

        rows = 4 * head_dim + 2 * mlp
        plane = plane_of(dp)
        side = max(plane)
        q_cols = q_scale.astype(f32).reshape(-1, head_dim, 1)
        k_cols = k_scale.astype(f32).reshape(-1, head_dim, 1)
        turned = [jnp.swapaxes(weight, 1, 2) for weight in (w_query, w_key, w_value)]
        vmem = pl.BlockSpec(memory_space=pltpu.VMEM)
        hbm = pl.BlockSpec(memory_space=pl.ANY)
        dma = pltpu.SemaphoreType.DMA
        flops = 2 * n_tokens * model_dim * (rows + seq_len // 2)
        middle, w_all, b_all = pl.pallas_call(
            functools.partial(first_kernel, seq_len, head_dim, tp, dp),
            out_shape=(
                jax.ShapeDtypeStruct((share, model_dim), bf16),
                jax.ShapeDtypeStruct((tp * rows, model_dim), bf16),
                jax.ShapeDtypeStruct((tp, 8, mlp), f32),
            ),
            in_specs=[hbm] * 7 + [vmem] * 6,
            out_specs=(vmem, hbm, vmem),
            scratch_shapes=[
                pltpu.VMEM((2, rows, model_dim), bf16), pltpu.VMEM((2, model_dim, mlp), bf16),
                pltpu.VMEM((2, share, model_dim), bf16),
                pltpu.VMEM((chips, 2, 2, half // 2, model_dim), bf16),
                pltpu.VMEM((tp, half, model_dim), bf16),
                pltpu.VMEM((tp, half, model_dim), bf16),
                pltpu.VMEM((4, half, model_dim), bf16),
                dma((2, 6)), dma, dma((2, 2)), dma((chips - 1, 2, 2)), dma((chips - 1, 2, 2)), dma((tp,)), dma((tp,)),
                dma((chips, 2)), dma((chips, 2)), dma((chips,)), dma((chips,)),
                dma((chips, 2, side)), dma((chips, 2, side)), dma((chips, 2, side, side)), dma((chips, 2, side, side)),
                dma((chips,)), dma((chips,)), dma((chips,)), dma((chips,)),
            ],
            compiler_params=pltpu.CompilerParams(vmem_limit_bytes=FIRST_VMEM, collective_id=0, has_side_effects=True),
            cost_estimate=pl.CostEstimate(flops=flops, bytes_accessed=4 * n_tokens * model_dim, transcendentals=0),
            name="first_layer",
        )(tokens, *turned, w_up, w_down, w_out, ln_scale, b_up, q_cols, k_cols, b_out, b_down)
        out = pl.pallas_call(
            functools.partial(second_kernel, seq_len, head_dim, tp),
            out_shape=jax.ShapeDtypeStruct((n_tokens, model_dim), bf16),
            in_specs=[vmem, hbm] + [vmem] * 6,
            out_specs=vmem,
            scratch_shapes=[
                pltpu.VMEM((2, rows, model_dim), bf16),
                pltpu.VMEM((share, model_dim), bf16), pltpu.VMEM((share, model_dim), f32),
                dma((2,)), dma((images, 2, 2, chips)), dma((images, 2, 2, chips)), dma((images, 2, 2, chips)), dma((images, 2, 2, chips)),
            ],
            compiler_params=pltpu.CompilerParams(vmem_limit_bytes=SECOND_VMEM, collective_id=1, has_side_effects=True),
            cost_estimate=pl.CostEstimate(flops=flops, bytes_accessed=2 * tp * rows * model_dim, transcendentals=0),
            name="second_layer",
        )(middle, w_all, b_all, ln_scale, b_out, b_down, q_cols, k_cols)
        return out.reshape(n_images, seq_len, model_dim)

    return jax.shard_map(per_device, mesh=mesh, in_specs=in_specs, out_specs=P("dp", None, None), check_vma=False)
```

```python
import functools
import math

import jax
import jax.numpy as jnp
from jax import lax
from jax.experimental import pallas as pl
from jax.experimental.pallas import tpu as pltpu
from jax.sharding import PartitionSpec as P

LN_EPS = 1e-6
LOG2E = 1.4426950408889634
VMEM_BYTES = 45 * 1024 * 1024
LEAD = 3
MESH = pl.DeviceIdType.MESH


def norm_rows(values, scale_row):
    mean_val = jnp.mean(values, axis=-1, keepdims=True)
    centered = values - mean_val
    variance = jnp.mean(centered * centered, axis=-1, keepdims=True)
    return (centered * lax.rsqrt(variance + LN_EPS) * scale_row).astype(jnp.bfloat16)


def norm_cols(values, scale_col):
    mean_val = jnp.mean(values, axis=0, keepdims=True)
    centered = values - mean_val
    variance = jnp.mean(centered * centered, axis=0, keepdims=True)
    return (centered * lax.rsqrt(variance + LN_EPS) * scale_col).astype(jnp.bfloat16)


def branches(normed, w_ref, b_up, q_col, k_col, seq_len, head_dim):
    tokens = normed.shape[0]
    mlp = b_up.shape[1]
    qkv = 3 * head_dim
    up_end = qkv + mlp
    proj = lax.dot_general(w_ref[0:qkv], normed, (((1,), (1,)), ((), ())), preferred_element_type=jnp.float32)
    queries = norm_cols(proj[0:head_dim], q_col)
    keys_all = norm_cols(proj[head_dim : 2 * head_dim], k_col)
    values_all = proj[2 * head_dim : qkv].astype(jnp.bfloat16)
    pre_act = lax.dot_general(normed, w_ref[qkv:up_end], (((1,), (1,)), ((), ())), preferred_element_type=jnp.float32)
    activated = jax.nn.gelu(pre_act + b_up, approximate=True).astype(jnp.bfloat16)
    mixed = []
    for img in range(tokens // seq_len):
        cols = slice(img * seq_len, (img + 1) * seq_len)
        scores = lax.dot_general(keys_all[:, cols], queries[:, cols], (((0,), (0,)), ((), ())), preferred_element_type=jnp.float32)
        top = jnp.max(scores, axis=0, keepdims=True)
        expd = jnp.exp2((scores - top) * (LOG2E * head_dim**-0.5))
        prob = (expd * (1.0 / jnp.sum(expd, axis=0, keepdims=True))).astype(jnp.bfloat16)
        mixed.append(jnp.dot(values_all[:, cols], prob, preferred_element_type=jnp.float32))
    mixed_rows = jnp.concatenate(mixed, axis=1).T.astype(jnp.bfloat16)
    both = jnp.concatenate([activated, mixed_rows], axis=1)
    return jnp.dot(both, w_ref[up_end:], preferred_element_type=jnp.float32)


def neighbours(tp):
    me = lax.axis_index("tp")
    chips = tp // 2
    core = lax.rem(me, 2)
    chip = me // 2
    right = lax.rem(chip + 1, chips) * 2 + core
    left = lax.rem(chip + chips - 1, chips) * 2 + core
    return core, chip, right, left, me + 1 - 2 * core


def enter(peers):
    barrier = pltpu.get_barrier_semaphore()
    for axis, peer in peers:
        pl.semaphore_signal(barrier, inc=1, device_id={axis: peer}, device_id_type=MESH)
    pl.semaphore_wait(barrier, len(peers))


def plane_of(dp):
    side = math.isqrt(dp)
    return (side, side) if side * side == dp else (1, dp)


def shard_of_round(chip, chips, number):
    sign = 1 - 2 * (number % 2)
    return lax.rem(chip + chips + sign * ((number + 1) // 2), chips)


def schedule_of(chips, plane):
    side = max(plane)
    events = {0: [("pass", 0, 0), ("pair", 0, 0)]}
    for number in range(1, chips):
        begin = 4 + (7 * (number - 1)) // 2 if side < 3 else 3 * number
        events.setdefault(begin, []).append(("pass", number, 0))
        for hop in range(1, side):
            events.setdefault(begin + 2 + hop, []).append(("line", number, hop))
        for hop in range(1, side):
            events.setdefault(begin + 2 + side + hop, []).append(("plane", number, hop))
        events.setdefault(begin + 1 + 2 * side, []).append(("pair", number, 0))
    return events


def layers_kernel(
    seq_len, head_dim, tp, dp,
    x_hbm, wq_hbm, wk_hbm, wv_hbm, wup_hbm, wdown_hbm, wout_hbm, ln_hbm, bo_hbm, bd_hbm, bup_hbm, q_hbm, k_hbm,
    out_ref, w_all,
    ln_ref, bo_ref, bd_ref, bup_ref, q_ref, k_ref, pack, up_raw, x_buf, own_x, ring, from_partner, to_partner, mine, b_all, w_buf, h_ref, acc_ref,
    load_sem, small_sem, own_sem, x_sem, ring_send, ring_recv, pair_send, pair_recv, z_send, z_recv, zb_send, zb_recv,
    line_send, line_recv, plane_send, plane_recv, w_send, w_recv, wb_send, wb_recv, wl_sem, out_send, out_recv, outp_send, outp_recv,
):
    core, chip, right, left, partner = neighbours(tp)
    chips = tp // 2
    me = 2 * chip + core
    rows = pack.shape[1]
    mlp = up_raw.shape[2]
    qkv = 3 * head_dim
    share = own_x.shape[0]
    images = share // seq_len
    quarter = seq_len // 4
    half = seq_len // 2
    f32 = jnp.float32
    plane = plane_of(dp)
    group = lax.axis_index("dp")
    at = (group // plane[1], lax.rem(group, plane[1]))
    unit = rows // (2 * dp)

    def group_at(axis, pos, other):
        return pos * plane[1] + other if axis == 0 else other * plane[1] + pos

    def beside(axis, sign):
        return group_at(axis, lax.rem(at[axis] + plane[axis] + sign, plane[axis]), at[1 - axis])

    def loads(layer):
        pieces = [(wq_hbm, pack.at[layer, 0:head_dim]), (wk_hbm, pack.at[layer, head_dim : 2 * head_dim]), (wv_hbm, pack.at[layer, 2 * head_dim : qkv]), (wup_hbm, up_raw.at[layer]), (wdown_hbm, pack.at[layer, qkv + mlp : qkv + 2 * mlp]), (wout_hbm, pack.at[layer, qkv + 2 * mlp : rows])]
        return [pltpu.make_async_copy(src.at[layer], dst, load_sem.at[layer, place]) for place, (src, dst) in enumerate(pieces)]

    def turn_up(layer):
        for copy in loads(layer):
            copy.wait()
        pack[layer, qkv : qkv + mlp] = up_raw[layer].T

    small = [(ln_hbm, ln_ref), (bo_hbm, bo_ref), (bd_hbm, bd_ref), (bup_hbm, bup_ref), (q_hbm, q_ref), (k_hbm, k_ref)]
    small = [pltpu.make_async_copy(src, dst, small_sem.at[place]) for place, (src, dst) in enumerate(small)]

    def column(ref, layer):
        row = ref[layer : layer + 1].astype(f32)
        return jnp.broadcast_to(row, (8, head_dim)).T[:, 0:1]

    def block(number, start, count, owner):
        base = (2 * shard_of_round(chip, chips, number) + owner) * rows + start
        return w_all.at[pl.ds(pl.multiple_of(base, 8), count)]

    def z_copies(number):
        copies = []
        for part in range(2):
            rightwards = (part == 0) if number == chips - 1 else number % 2 == 1
            hops = (number + 1) // 2
            source = lax.rem(chip + chips + (1 - hops if rightwards else hops - 1), chips)
            peer = right if rightwards else left
            ref = w_all.at[pl.ds(pl.multiple_of((2 * source + core) * rows + (part * dp + group) * unit, 8), unit)]
            copies.append(pltpu.make_async_remote_copy(src_ref=ref, dst_ref=ref, send_sem=z_send.at[number, part], recv_sem=z_recv.at[number, part], device_id={"tp": peer}, device_id_type=MESH))
            if part == 0:
                ref = b_all.at[2 * source + core]
                copies.append(pltpu.make_async_remote_copy(src_ref=ref, dst_ref=ref, send_sem=zb_send.at[number], recv_sem=zb_recv.at[number], device_id={"tp": peer}, device_id_type=MESH))
        return copies

    def z_onward(number):
        if number == 0:
            return [(later, (0, 1)) for later in (1, 2) if later < chips - 1] or [(chips - 1, (0, 1))]
        if number + 2 < chips - 1:
            return [(number + 2, (0, 1))]
        if number < chips - 1:
            return [(chips - 1, (number % 2 == 0,))]
        return []

    def z_start(later, parts):
        copies = z_copies(later)
        for part in parts:
            if part == 0:
                copies[0].start()
                copies[1].start()
            else:
                copies[2].start()

    def axes(part):
        return (0, 1) if part == 0 else (1, 0)

    def sign_of(number):
        return 1 - 2 * (number % 2)

    def line_copy(number, part, hop):
        axis, sign = axes(part)[0], sign_of(number)
        source = group_at(axis, lax.rem(at[axis] + plane[axis] - sign * hop, plane[axis]), at[1 - axis])
        ref = block(number, (part * dp + source) * unit, unit, core)
        return pltpu.make_async_remote_copy(src_ref=ref, dst_ref=ref, send_sem=line_send.at[number, part, hop], recv_sem=line_recv.at[number, part, hop], device_id={"dp": beside(axis, sign)}, device_id_type=MESH)

    def plane_copy(number, part, off, hop):
        (one, two), sign = axes(part), sign_of(number)
        source = group_at(one, lax.rem(at[one] + plane[one] - sign * off, plane[one]), lax.rem(at[two] + plane[two] - sign * hop, plane[two]))
        ref = block(number, (part * dp + source) * unit, unit, core)
        return pltpu.make_async_remote_copy(src_ref=ref, dst_ref=ref, send_sem=plane_send.at[number, part, off, hop], recv_sem=plane_recv.at[number, part, off, hop], device_id={"dp": beside(two, sign)}, device_id_type=MESH)

    def w_pair(number, who):
        ref = block(number, 0, rows, who)
        bias = b_all.at[2 * shard_of_round(chip, chips, number) + who]
        return [
            pltpu.make_async_remote_copy(src_ref=ref, dst_ref=ref, send_sem=w_send.at[number], recv_sem=w_recv.at[number], device_id={"tp": partner}, device_id_type=MESH),
            pltpu.make_async_remote_copy(src_ref=bias, dst_ref=bias, send_sem=wb_send.at[number], recv_sem=wb_recv.at[number], device_id={"tp": partner}, device_id_type=MESH),
        ]

    def gather(kind, number, hop):
        if kind == "pass":
            if number > 0:
                for copy in z_copies(number):
                    copy.wait_recv()
            for later, parts in z_onward(number):
                z_start(later, parts)
            for part in range(2):
                if number > 0 and plane[axes(part)[0]] > 1:
                    line_copy(number, part, 0).start()
            for part in range(2):
                if number > 0 and plane[axes(part)[1]] > 1:
                    plane_copy(number, part, 0, 0).start()
        for part in range(2):
            one, two = (plane[axis] for axis in axes(part))
            if kind == "line" and hop < one:
                line_copy(number, part, hop - 1).wait_recv()
                if hop < one - 1:
                    line_copy(number, part, hop).start()
                if two > 1:
                    plane_copy(number, part, hop, 0).start()
            if kind == "plane" and hop < two:
                for off in range(one):
                    plane_copy(number, part, off, hop - 1).wait_recv()
                    if hop < two - 1:
                        plane_copy(number, part, off, hop).start()
        if kind == "pair":
            for copy in w_pair(number, core):
                copy.start()

    def place_of(item):
        image, number = item // chips, lax.rem(item, chips)
        near, odd, own = number // 2, lax.rem(number, 2), number // (chips - 1)
        far = chips - 2 - near
        there = lax.rem(chip + 2 * chips + (2 * odd - 1) * (1 + near) * (1 - own), chips)
        upper = (near * (1 - odd) + far * odd) * (1 - own) + (chips - 1) * own
        lower = (near * odd + far * (1 - odd)) * (1 - own) + (chips - 1) * own
        return image, there, (upper, lower)

    def x_copies(item):
        image, there, _ = place_of(item)
        slot = lax.rem(item, 2)
        return [
            pltpu.make_async_copy(
                x_hbm.at[pl.ds(pl.multiple_of((2 * there + owner) * share + image * seq_len, seq_len), seq_len)],
                x_buf.at[slot, pl.ds(place * seq_len, seq_len)],
                x_sem.at[slot, place],
            )
            for place, owner in ((0, 1 - core), (1, core))
        ]

    def pair_copies(item):
        image, _, steps = place_of(item)
        return [
            pltpu.make_async_remote_copy(
                src_ref=to_partner.at[lax.rem(item, 4), way], dst_ref=from_partner.at[image, way, steps[way]],
                send_sem=pair_send.at[image, way, steps[way]], recv_sem=pair_recv.at[image, way, steps[way]],
                device_id={"tp": partner}, device_id_type=MESH,
            )
            for way in range(2)
        ]

    def pair_arrival(image, way, step):
        return pltpu.make_async_remote_copy(
            src_ref=to_partner.at[0, way], dst_ref=from_partner.at[image, way, step],
            send_sem=pair_send.at[image, way, step], recv_sem=pair_recv.at[image, way, step],
            device_id={"tp": partner}, device_id_type=MESH,
        )

    def ring_copy(image, step, way, sub):
        return pltpu.make_async_remote_copy(
            src_ref=ring.at[image, step, way, sub], dst_ref=ring.at[image, step + 1, way, sub],
            send_sem=ring_send.at[image, step, way, sub], recv_sem=ring_recv.at[image, step, way, sub],
            device_id={"tp": left if way else right}, device_id_type=MESH,
        )

    def w_copy(turn):
        shard = lax.rem(turn, tp)
        slot = lax.rem(turn, 2)
        return pltpu.make_async_copy(block(shard // 2, 0, rows, whose(shard)), w_buf.at[slot], wl_sem.at[slot])

    def whose(shard):
        odd = lax.rem(shard, 2)
        return core + odd - 2 * core * odd

    def chunk(image, way, sub, owner):
        offset = owner * share + image * seq_len + way * (2 * quarter) + sub * quarter
        return out_ref.at[pl.ds(pl.multiple_of(offset, quarter), quarter)]

    def origin(way, step):
        back = chip - step if way == 0 else chip + step
        return 2 * lax.rem(back + chips, chips)

    def out_copy(image, way, sub, step):
        ref = chunk(image, way, sub, origin(way, step) + core)
        return pltpu.make_async_remote_copy(
            src_ref=ref, dst_ref=ref, send_sem=out_send.at[image, way, sub, step], recv_sem=out_recv.at[image, way, sub, step],
            device_id={"tp": left if way else right}, device_id_type=MESH,
        )

    def arrival(image, way, sub, step):
        ref = chunk(image, way, sub, origin(way, step + 1) + core)
        return pltpu.make_async_remote_copy(
            src_ref=ref, dst_ref=ref, send_sem=out_send.at[image, way, sub, step], recv_sem=out_recv.at[image, way, sub, step],
            device_id={"tp": left if way else right}, device_id_type=MESH,
        )

    def out_pair(image, way, sub, step, who):
        ref = chunk(image, way, sub, origin(way, step) + who)
        return pltpu.make_async_remote_copy(
            src_ref=ref, dst_ref=ref, send_sem=outp_send.at[image, way, sub, step], recv_sem=outp_recv.at[image, way, sub, step],
            device_id={"tp": partner}, device_id_type=MESH,
        )

    def event(image, number):
        step = number // 2
        sub = lax.rem(number, 2)
        for way in range(2):
            arrival(image, way, sub, step).wait_recv()

            @pl.when(step + 1 < chips - 1)
            def _():
                out_copy(image, way, sub, step + 1).start()

            out_pair(image, way, sub, step + 1, core).start()

    peers = [("tp", right), ("tp", left), ("tp", partner)]
    for axis in range(2):
        peers += [("dp", beside(axis, sign)) for sign in (1, -1)[: min(plane[axis] - 1, 2)]]
    enter(peers)

    for layer in (1, 0):
        for copy in loads(layer):
            copy.start()
        if layer == 1:
            for copy in small:
                copy.start()
    for copy in x_copies(0):
        copy.start()
    own_load = pltpu.make_async_copy(x_hbm.at[pl.ds(pl.multiple_of(me * share, share), share)], own_x, own_sem.at[1])
    own_load.start()
    for copy in small:
        copy.wait()
    b_all[me] = jnp.broadcast_to(bup_ref[1:2].astype(f32), b_all.shape[1:])
    turn_up(1)
    own_copy = pltpu.make_async_copy(pack.at[1], w_all.at[pl.ds(pl.multiple_of(me * rows, 8), rows)], own_sem.at[0])
    own_copy.start()
    turn_up(0)
    own_copy.wait()
    own_load.wait()
    events = schedule_of(chips, plane)
    ln_rows = [ln_ref[layer : layer + 1].astype(f32) for layer in range(2)]
    bias_rows = [bo_ref[layer : layer + 1].astype(f32) + bd_ref[layer : layer + 1].astype(f32) for layer in range(2)]
    b_row = bup_ref[0:1].astype(f32)
    q_cols = [column(q_ref, layer) for layer in range(2)]
    k_cols = [column(k_ref, layer) for layer in range(2)]
    items = images * chips
    ready = [due - 2 * number + 1 for due, due_events in events.items() for kind, number, _ in due_events if kind == "pair"]
    second = max([LEAD + items] + ready)

    def turn(index, carry):
        t = index - LEAD

        @pl.when(jnp.logical_and(t >= 0, t < 2 * items))
        def _():
            image = t // (2 * chips)
            step = lax.rem(t, 2 * chips) // 2
            sub = lax.rem(t, 2)
            span = pl.ds(pl.multiple_of(sub * quarter, quarter), quarter)
            for way in range(2):
                @pl.when(sub == 0)
                def _():
                    pair_arrival(image, way, step).wait_recv()

                local = from_partner[image, way, step, span].astype(f32) + mine[image, way, step, span].astype(f32)

                @pl.when(step == 0)
                def _():
                    ring[image, 0, way, sub] = local.astype(ring.dtype)

                @pl.when(step > 0)
                def _():
                    ring_copy(image, step - 1, way, sub).wait_recv()

                @pl.when(jnp.logical_and(step > 0, step < chips - 1))
                def _():
                    ring[image, step, way, sub] = (ring[image, step, way, sub].astype(f32) + local).astype(ring.dtype)

                @pl.when(step < chips - 1)
                def _():
                    ring_copy(image, step, way, sub).start()

                @pl.when(step == chips - 1)
                def _():
                    here = pl.ds(pl.multiple_of(image * seq_len + way * half + sub * quarter, quarter), quarter)
                    total = ring[image, chips - 1, way, sub].astype(f32) + local
                    middle = (own_x[here].astype(f32) + bias_rows[0] + total).astype(jnp.bfloat16).astype(f32)
                    h_ref[here] = norm_rows(middle, ln_rows[1])
                    acc_ref[here] = middle + bias_rows[1]

        for due, due_events in sorted(events.items()):
            @pl.when(index == due)
            def _():
                for event_args in due_events:
                    gather(*event_args)

        @pl.when(index < items)
        def _():
            @pl.when(index + 1 < items)
            def _():
                for copy in x_copies(index + 1):
                    copy.start()

            @pl.when(index >= 4)
            def _():
                for copy in pair_copies(index - 4):
                    copy.wait_send()

            for copy in x_copies(index):
                copy.wait()
            normed = norm_rows(x_buf[lax.rem(index, 2)].astype(f32), ln_rows[0])
            part = branches(normed, pack.at[0], b_row, q_cols[0], k_cols[0], seq_len, head_dim).astype(jnp.bfloat16)
            image, _, steps = place_of(index)
            for way in range(2):
                to_partner[lax.rem(index, 4), way] = part[way * half : (way + 1) * half]
                mine[image, way, steps[way]] = part[seq_len + way * half : seq_len + (way + 1) * half]
            for copy in pair_copies(index):
                copy.start()

        @pl.when(index == second - 1)
        def _():
            w_copy(0).start()

        @pl.when(index >= second)
        def _():
            m = index - second
            image = m // tp
            shard = lax.rem(m, tp)

            @pl.when(jnp.logical_and(image > 0, lax.rem(shard, 2) == 0))
            def _():
                event(image - 1, shard // 2)

            for number in range(chips):
                @pl.when(m == 2 * number)
                def _():
                    for copy in w_pair(number, 1 - core):
                        copy.wait_recv()

            @pl.when(m + 1 < images * tp)
            def _():
                w_copy(m + 1).start()

            w_copy(m).wait()
            slot = lax.rem(m, 2)
            span = pl.ds(pl.multiple_of(image * seq_len, seq_len), seq_len)
            owner = 2 * shard_of_round(chip, chips, shard // 2) + whose(shard)
            acc_ref[span] += branches(h_ref[span], w_buf.at[slot], b_all[owner][0:1], q_cols[1], k_cols[1], seq_len, head_dim)

            @pl.when(shard == tp - 1)
            def _():
                out_ref[pl.ds(pl.multiple_of(me * share + image * seq_len, seq_len), seq_len)] = acc_ref[span].astype(out_ref.dtype)
                for sub in range(2):
                    for way in range(2):
                        out_copy(image, way, sub, 0).start()
                for sub in range(2):
                    for way in range(2):
                        out_pair(image, way, sub, 0, core).start()

        return carry

    lax.fori_loop(0, second + images * tp, turn, 0)
    total = 2 * (chips - 1)
    done = tp // 2

    def tail(number, carry):
        @pl.when(number + done < total)
        def _():
            event(images - 2, number + done)

        event(images - 1, number)
        return carry

    lax.fori_loop(0, total, tail, 0)

    def drain(step, carry):
        for image in range(images):
            for way in range(2):
                for sub in range(2):
                    @pl.when(step < chips - 1)
                    def _():
                        ring_copy(image, step, way, sub).wait_send()
                        out_copy(image, way, sub, step).wait_send()

                    out_pair(image, way, sub, step, core).wait_send()
                    out_pair(image, way, sub, step, 1 - core).wait_recv()
        return carry

    lax.fori_loop(0, chips, drain, 0)
    for item in range(max(items - 4, 0), items):
        for copy in pair_copies(item):
            copy.wait_send()
    for number in range(chips):
        for copy in w_pair(number, core):
            copy.wait_send()
        for part in range(2 if number > 0 else 0):
            one, two = (plane[axis] for axis in axes(part))
            for hop in range(one - 1):
                line_copy(number, part, hop).wait_send()
            for hop in range(two - 1):
                for off in range(one):
                    plane_copy(number, part, off, hop).wait_send()
        if number > 0:
            for copy in z_copies(number):
                copy.wait_send()


def solution(mesh):
    col_spec = P(None, None, "tp")
    row_spec = P(None, "tp", None)
    in_specs = (P("dp", None, None), P(), col_spec, col_spec, col_spec, P(), P(), row_spec, P(), col_spec, P(None, "tp"), row_spec, P())
    tp = mesh.shape["tp"]
    dp = mesh.shape["dp"]
    chips = tp // 2

    def per_device(tokens_in, ln_scale, w_query, w_key, w_value, q_scale, k_scale, w_out, b_out, w_up, b_up, w_down, b_down):
        n_images, seq_len, model_dim = tokens_in.shape
        n_tokens = n_images * seq_len
        head_dim = q_scale.shape[1]
        mlp = w_up.shape[2]
        share = n_tokens // tp
        images = share // seq_len
        half, quarter = seq_len // 2, seq_len // 4
        rows = 4 * head_dim + 2 * mlp
        side = max(plane_of(dp))
        bf16, f32 = jnp.bfloat16, jnp.float32
        turned = [jnp.swapaxes(weight, 1, 2) for weight in (w_query, w_key, w_value)]
        hbm = pl.BlockSpec(memory_space=pltpu.HBM)
        vmem, dma = pltpu.VMEM, pltpu.SemaphoreType.DMA
        layers = ln_scale.shape[0]
        operands = (tokens_in.reshape(n_tokens, model_dim), *turned, w_up, w_down, w_out, ln_scale, b_out, b_down, b_up, q_scale, k_scale)
        out, _ = pl.pallas_call(
            functools.partial(layers_kernel, seq_len, head_dim, tp, dp),
            out_shape=(vmem((n_tokens, model_dim), bf16), jax.ShapeDtypeStruct((tp * rows, model_dim), bf16)),
            in_specs=[hbm] * 13,
            out_specs=(pl.BlockSpec(memory_space=pltpu.VMEM), hbm),
            scratch_shapes=[
                vmem((layers, model_dim), bf16), vmem((layers, model_dim), bf16), vmem((layers, model_dim), bf16), vmem((layers, mlp), bf16), vmem((layers, head_dim), bf16), vmem((layers, head_dim), bf16),
                vmem((layers, rows, model_dim), bf16), vmem((layers, model_dim, mlp), bf16),
                vmem((2, 2 * seq_len, model_dim), bf16), vmem((share, model_dim), bf16),
                vmem((images, chips, 2, 2, quarter, model_dim), bf16),
                vmem((images, 2, chips, half, model_dim), bf16), vmem((4, 2, half, model_dim), bf16), vmem((images, 2, chips, half, model_dim), bf16),
                vmem((tp, 8, mlp), f32), vmem((2, rows, model_dim), bf16), vmem((share, model_dim), bf16), vmem((share, model_dim), f32),
                dma((layers, 6)), dma((6,)), dma((2,)), dma((2, 2)),
                dma((images, chips, 2, 2)), dma((images, chips, 2, 2)), dma((images, 2, chips)), dma((images, 2, chips)),
                dma((chips, 2)), dma((chips, 2)), dma((chips,)), dma((chips,)),
                dma((chips, 2, side)), dma((chips, 2, side)), dma((chips, 2, side, side)), dma((chips, 2, side, side)),
                dma((chips,)), dma((chips,)), dma((chips,)), dma((chips,)), dma((2,)),
                dma((images, 2, 2, chips)), dma((images, 2, 2, chips)), dma((images, 2, 2, chips)), dma((images, 2, 2, chips)),
            ],
            compiler_params=pltpu.CompilerParams(vmem_limit_bytes=VMEM_BYTES, collective_id=0, has_side_effects=True),
            cost_estimate=pl.CostEstimate(flops=4 * n_tokens * model_dim * (rows + seq_len // 2), bytes_accessed=8 * n_tokens * model_dim, transcendentals=0),
            name="layers",
        )(*(pltpu.with_memory_space_constraint(value, pltpu.HBM) for value in operands))
        return out.reshape(n_images, seq_len, model_dim)

    return jax.shard_map(per_device, mesh=mesh, in_specs=in_specs, out_specs=P("dp", None, None), check_vma=False)
```

```python
import functools
import math

import jax
import jax.numpy as jnp
from jax import lax
from jax.experimental import pallas as pl
from jax.experimental.pallas import tpu as pltpu
from jax.sharding import PartitionSpec as P

LN_EPS = 1e-6
LOG2E = 1.4426950408889634
VMEM_BYTES = 45 * 1024 * 1024
LEAD = 3
MESH = pl.DeviceIdType.MESH


def norm_rows(values, scale_row):
    mean_val = jnp.mean(values, axis=-1, keepdims=True)
    centered = values - mean_val
    variance = jnp.mean(centered * centered, axis=-1, keepdims=True)
    return (centered * lax.rsqrt(variance + LN_EPS) * scale_row).astype(jnp.bfloat16)


def norm_cols(values, scale_col):
    mean_val = jnp.mean(values, axis=0, keepdims=True)
    centered = values - mean_val
    variance = jnp.mean(centered * centered, axis=0, keepdims=True)
    return (centered * lax.rsqrt(variance + LN_EPS) * scale_col).astype(jnp.bfloat16)


def branches(normed, w_ref, b_up, q_col, k_col, seq_len, head_dim):
    tokens = normed.shape[0]
    mlp = b_up.shape[1]
    qkv = 3 * head_dim
    up_end = qkv + mlp
    proj = lax.dot_general(w_ref[0:qkv], normed, (((1,), (1,)), ((), ())), preferred_element_type=jnp.float32)
    queries = norm_cols(proj[0:head_dim], q_col)
    keys_all = norm_cols(proj[head_dim : 2 * head_dim], k_col)
    values_all = proj[2 * head_dim : qkv].astype(jnp.bfloat16)
    pre_act = lax.dot_general(normed, w_ref[qkv:up_end], (((1,), (1,)), ((), ())), preferred_element_type=jnp.float32)
    activated = jax.nn.gelu(pre_act + b_up, approximate=True).astype(jnp.bfloat16)
    mixed = []
    for img in range(tokens // seq_len):
        cols = slice(img * seq_len, (img + 1) * seq_len)
        scores = lax.dot_general(keys_all[:, cols], queries[:, cols], (((0,), (0,)), ((), ())), preferred_element_type=jnp.float32)
        top = jnp.max(scores, axis=0, keepdims=True)
        expd = jnp.exp2((scores - top) * (LOG2E * head_dim**-0.5))
        prob = (expd * (1.0 / jnp.sum(expd, axis=0, keepdims=True))).astype(jnp.bfloat16)
        mixed.append(jnp.dot(values_all[:, cols], prob, preferred_element_type=jnp.float32))
    mixed_rows = jnp.concatenate(mixed, axis=1).T.astype(jnp.bfloat16)
    both = jnp.concatenate([activated, mixed_rows], axis=1)
    return jnp.dot(both, w_ref[up_end:], preferred_element_type=jnp.float32)


def neighbours(tp):
    me = lax.axis_index("tp")
    chips = tp // 2
    core = lax.rem(me, 2)
    chip = me // 2
    right = lax.rem(chip + 1, chips) * 2 + core
    left = lax.rem(chip + chips - 1, chips) * 2 + core
    return core, chip, right, left, me + 1 - 2 * core


def enter(peers):
    barrier = pltpu.get_barrier_semaphore()
    for axis, peer in peers:
        pl.semaphore_signal(barrier, inc=1, device_id={axis: peer}, device_id_type=MESH)
    pl.semaphore_wait(barrier, len(peers))


def plane_of(dp):
    side = math.isqrt(dp)
    return (side, side) if side * side == dp else (1, dp)


def shard_of_round(chip, chips, number):
    sign = 1 - 2 * (number % 2)
    return lax.rem(chip + chips + sign * ((number + 1) // 2), chips)


def schedule_of(chips, plane):
    side = max(plane)
    events = {}
    for number in range(1, chips):
        begin = 4 + ((7 * (number - 1) + 1) // 2 if side < 3 else 3 * (number - 1))
        if number % 2 == 1:
            pair = (number + 1) // 2
            events.setdefault(begin, []).extend([("came", pair, 0), ("onward", pair, 0)])
            events.setdefault(begin + 2, []).append(("onward", pair, 1))
        events.setdefault(begin, []).append(("pass", number, 0))
        for hop in range(1, side):
            events.setdefault(begin + 1 + hop, []).append(("line", number, hop))
        for hop in range(1, side):
            events.setdefault(begin + 2 + side + hop, []).append(("plane", number, hop))
        events.setdefault(begin + 1 + 2 * side, []).append(("pair", number, 0))
    return events


def layers_kernel(
    seq_len, head_dim, tp, dp,
    x_hbm, wq_hbm, wk_hbm, wv_hbm, wup_hbm, wdown_hbm, wout_hbm, ln_hbm, bo_hbm, bd_hbm, bup_hbm, q_hbm, k_hbm,
    out_ref, w_all,
    ln_ref, bo_ref, bd_ref, bup_ref, q_ref, k_ref, pack, up_raw, x_buf, own_x, ring, from_partner, to_partner, mine, b_all, w_buf, h_ref, acc_ref,
    load_sem, small_sem, own_sem, x_sem, ring_send, ring_recv, pair_send, pair_recv, z_send, z_recv, zb_send, zb_recv,
    line_send, line_recv, plane_send, plane_recv, w_send, w_recv, wb_send, wb_recv, wl_sem, out_send, out_recv, outp_send, outp_recv,
):
    core, chip, right, left, partner = neighbours(tp)
    chips = tp // 2
    me = 2 * chip + core
    rows = pack.shape[1]
    mlp = up_raw.shape[2]
    qkv = 3 * head_dim
    share = own_x.shape[0]
    images = share // seq_len
    quarter = seq_len // 4
    half = seq_len // 2
    f32 = jnp.float32
    plane = plane_of(dp)
    group = lax.axis_index("dp")
    at = (group // plane[1], lax.rem(group, plane[1]))
    unit = rows // (2 * dp)

    def group_at(axis, pos, other):
        return pos * plane[1] + other if axis == 0 else other * plane[1] + pos

    def beside(axis, sign):
        return group_at(axis, lax.rem(at[axis] + plane[axis] + sign, plane[axis]), at[1 - axis])

    def loads(layer):
        pieces = [(wq_hbm, pack.at[layer, 0:head_dim]), (wk_hbm, pack.at[layer, head_dim : 2 * head_dim]), (wv_hbm, pack.at[layer, 2 * head_dim : qkv]), (wup_hbm, up_raw.at[layer]), (wdown_hbm, pack.at[layer, qkv + mlp : qkv + 2 * mlp]), (wout_hbm, pack.at[layer, qkv + 2 * mlp : rows])]
        return [pltpu.make_async_copy(src.at[layer], dst, load_sem.at[layer, place]) for place, (src, dst) in enumerate(pieces)]

    def turn_up(layer):
        for copy in loads(layer):
            copy.wait()
        pack[layer, qkv : qkv + mlp] = up_raw[layer].T

    small = [(ln_hbm, ln_ref), (bo_hbm, bo_ref), (bd_hbm, bd_ref), (bup_hbm, bup_ref), (q_hbm, q_ref), (k_hbm, k_ref)]
    small = [pltpu.make_async_copy(src, dst, small_sem.at[place]) for place, (src, dst) in enumerate(small)]

    def column(ref, layer):
        row = ref[layer : layer + 1].astype(f32)
        return jnp.broadcast_to(row, (8, head_dim)).T[:, 0:1]

    def block(number, start, count, owner):
        base = (2 * shard_of_round(chip, chips, number) + owner) * rows + start
        return w_all.at[pl.ds(pl.multiple_of(base, 8), count)]

    def z_copies(number):
        copies = []
        for part in range(2):
            rightwards = (part == 0) if number == chips - 1 else number % 2 == 1
            hops = (number + 1) // 2
            source = lax.rem(chip + chips + (1 - hops if rightwards else hops - 1), chips)
            peer = right if rightwards else left
            ref = w_all.at[pl.ds(pl.multiple_of((2 * source + core) * rows + (part * dp + group) * unit, 8), unit)]
            copies.append(pltpu.make_async_remote_copy(src_ref=ref, dst_ref=ref, send_sem=z_send.at[number, part], recv_sem=z_recv.at[number, part], device_id={"tp": peer}, device_id_type=MESH))
            if part == 0:
                ref = b_all.at[2 * source + core]
                copies.append(pltpu.make_async_remote_copy(src_ref=ref, dst_ref=ref, send_sem=zb_send.at[number], recv_sem=zb_recv.at[number], device_id={"tp": peer}, device_id_type=MESH))
        return copies

    def z_onward(number):
        if number == 0:
            return [(later, (0, 1)) for later in (1, 2) if later < chips - 1] or [(chips - 1, (0, 1))]
        if number + 2 < chips - 1:
            return [(number + 2, (0, 1))]
        if number < chips - 1:
            return [(chips - 1, (number % 2 == 0,))]
        return []

    def z_start(later, parts):
        copies = z_copies(later)
        for part in parts:
            if part == 0:
                copies[0].start()
                copies[1].start()
            else:
                copies[2].start()

    def axes(part):
        return (0, 1) if part == 0 else (1, 0)

    def sign_of(number):
        return 1 - 2 * (number % 2)

    def line_copy(number, part, hop):
        axis, sign = axes(part)[0], sign_of(number)
        source = group_at(axis, lax.rem(at[axis] + plane[axis] - sign * hop, plane[axis]), at[1 - axis])
        ref = block(number, (part * dp + source) * unit, unit, core)
        return pltpu.make_async_remote_copy(src_ref=ref, dst_ref=ref, send_sem=line_send.at[number, part, hop], recv_sem=line_recv.at[number, part, hop], device_id={"dp": beside(axis, sign)}, device_id_type=MESH)

    def plane_copy(number, part, off, hop):
        (one, two), sign = axes(part), sign_of(number)
        source = group_at(one, lax.rem(at[one] + plane[one] - sign * off, plane[one]), lax.rem(at[two] + plane[two] - sign * hop, plane[two]))
        ref = block(number, (part * dp + source) * unit, unit, core)
        return pltpu.make_async_remote_copy(src_ref=ref, dst_ref=ref, send_sem=plane_send.at[number, part, off, hop], recv_sem=plane_recv.at[number, part, off, hop], device_id={"dp": beside(two, sign)}, device_id_type=MESH)

    def w_pair(number, who):
        ref = block(number, 0, rows, who)
        bias = b_all.at[2 * shard_of_round(chip, chips, number) + who]
        return [
            pltpu.make_async_remote_copy(src_ref=ref, dst_ref=ref, send_sem=w_send.at[number], recv_sem=w_recv.at[number], device_id={"tp": partner}, device_id_type=MESH),
            pltpu.make_async_remote_copy(src_ref=bias, dst_ref=bias, send_sem=wb_send.at[number], recv_sem=wb_recv.at[number], device_id={"tp": partner}, device_id_type=MESH),
        ]

    def gather(kind, number, hop):
        both = [each for each in (2 * number - 1, 2 * number) if each < chips]
        if kind == "came":
            for each in both:
                for copy in z_copies(each):
                    copy.wait_recv()
        if kind == "onward":
            for each in both:
                for later, parts in z_onward(each):
                    if hop in parts:
                        z_start(later, (hop,))
        if kind == "pass":
            for part in range(2):
                if plane[axes(part)[0]] > 1:
                    line_copy(number, part, 0).start()
            for part in range(2):
                if plane[axes(part)[1]] > 1:
                    plane_copy(number, part, 0, 0).start()
        for part in range(2):
            one, two = (plane[axis] for axis in axes(part))
            if kind == "line" and hop < one:
                line_copy(number, part, hop - 1).wait_recv()
                if hop < one - 1:
                    line_copy(number, part, hop).start()
                if two > 1:
                    plane_copy(number, part, hop, 0).start()
            if kind == "plane" and hop < two:
                for off in range(one):
                    plane_copy(number, part, off, hop - 1).wait_recv()
                    if hop < two - 1:
                        plane_copy(number, part, off, hop).start()
        if kind == "pair":
            for copy in w_pair(number, core):
                copy.start()

    def place_of(item):
        image, number = item // chips, lax.rem(item, chips)
        near, odd, own = number // 2, lax.rem(number, 2), number // (chips - 1)
        far = chips - 2 - near
        there = lax.rem(chip + 2 * chips + (2 * odd - 1) * (1 + near) * (1 - own), chips)
        upper = (near * (1 - odd) + far * odd) * (1 - own) + (chips - 1) * own
        lower = (near * odd + far * (1 - odd)) * (1 - own) + (chips - 1) * own
        return image, there, (upper, lower)

    def x_copies(item):
        image, there, _ = place_of(item)
        slot = lax.rem(item, 2)
        return [
            pltpu.make_async_copy(
                x_hbm.at[pl.ds(pl.multiple_of((2 * there + owner) * share + image * seq_len, seq_len), seq_len)],
                x_buf.at[slot, pl.ds(place * seq_len, seq_len)],
                x_sem.at[slot, place],
            )
            for place, owner in ((0, 1 - core), (1, core))
        ]

    def pair_copies(item):
        image, _, steps = place_of(item)
        return [
            pltpu.make_async_remote_copy(
                src_ref=to_partner.at[lax.rem(item, 4), way], dst_ref=from_partner.at[image, way, steps[way]],
                send_sem=pair_send.at[image, way, steps[way]], recv_sem=pair_recv.at[image, way, steps[way]],
                device_id={"tp": partner}, device_id_type=MESH,
            )
            for way in range(2)
        ]

    def pair_arrival(image, way, step):
        return pltpu.make_async_remote_copy(
            src_ref=to_partner.at[0, way], dst_ref=from_partner.at[image, way, step],
            send_sem=pair_send.at[image, way, step], recv_sem=pair_recv.at[image, way, step],
            device_id={"tp": partner}, device_id_type=MESH,
        )

    def ring_copy(image, step, way, sub):
        return pltpu.make_async_remote_copy(
            src_ref=ring.at[image, step, way, sub], dst_ref=ring.at[image, step + 1, way, sub],
            send_sem=ring_send.at[image, step, way, sub], recv_sem=ring_recv.at[image, step, way, sub],
            device_id={"tp": left if way else right}, device_id_type=MESH,
        )

    def w_copy(turn):
        shard = lax.rem(turn, tp)
        slot = lax.rem(turn, 2)
        return pltpu.make_async_copy(block(shard // 2, 0, rows, whose(shard)), w_buf.at[slot], wl_sem.at[slot])

    def whose(shard):
        odd = lax.rem(shard, 2)
        return core + odd - 2 * core * odd

    def chunk(image, way, sub, owner):
        offset = owner * share + image * seq_len + way * (2 * quarter) + sub * quarter
        return out_ref.at[pl.ds(pl.multiple_of(offset, quarter), quarter)]

    def origin(way, step):
        back = chip - step if way == 0 else chip + step
        return 2 * lax.rem(back + chips, chips)

    def out_copy(image, way, sub, step):
        ref = chunk(image, way, sub, origin(way, step) + core)
        return pltpu.make_async_remote_copy(
            src_ref=ref, dst_ref=ref, send_sem=out_send.at[image, way, sub, step], recv_sem=out_recv.at[image, way, sub, step],
            device_id={"tp": left if way else right}, device_id_type=MESH,
        )

    def arrival(image, way, sub, step):
        ref = chunk(image, way, sub, origin(way, step + 1) + core)
        return pltpu.make_async_remote_copy(
            src_ref=ref, dst_ref=ref, send_sem=out_send.at[image, way, sub, step], recv_sem=out_recv.at[image, way, sub, step],
            device_id={"tp": left if way else right}, device_id_type=MESH,
        )

    def out_pair(image, way, sub, step, who):
        ref = chunk(image, way, sub, origin(way, step) + who)
        return pltpu.make_async_remote_copy(
            src_ref=ref, dst_ref=ref, send_sem=outp_send.at[image, way, sub, step], recv_sem=outp_recv.at[image, way, sub, step],
            device_id={"tp": partner}, device_id_type=MESH,
        )

    def event(image, number):
        step = number // 2
        sub = lax.rem(number, 2)
        for way in range(2):
            arrival(image, way, sub, step).wait_recv()

            @pl.when(step + 1 < chips - 1)
            def _():
                out_copy(image, way, sub, step + 1).start()

            out_pair(image, way, sub, step + 1, core).start()

    peers = [("tp", right), ("tp", left), ("tp", partner)]
    for axis in range(2):
        peers += [("dp", beside(axis, sign)) for sign in (1, -1)[: min(plane[axis] - 1, 2)]]
    enter(peers)

    for layer in (1, 0):
        for copy in loads(layer):
            copy.start()
        if layer == 1:
            for copy in small:
                copy.start()
    for copy in x_copies(0):
        copy.start()
    own_load = pltpu.make_async_copy(x_hbm.at[pl.ds(pl.multiple_of(me * share, share), share)], own_x, own_sem.at[1])
    own_load.start()
    for copy in small:
        copy.wait()
    b_all[me] = jnp.broadcast_to(bup_ref[1:2].astype(f32), b_all.shape[1:])
    turn_up(1)
    own_copy = pltpu.make_async_copy(pack.at[1], w_all.at[pl.ds(pl.multiple_of(me * rows, 8), rows)], own_sem.at[0])
    own_copy.start()
    own_copy.wait()
    for later, parts in z_onward(0):
        z_start(later, parts)
    gather("pair", 0, 0)
    turn_up(0)
    own_load.wait()
    events = schedule_of(chips, plane)
    ln_rows = [ln_ref[layer : layer + 1].astype(f32) for layer in range(2)]
    bias_rows = [bo_ref[layer : layer + 1].astype(f32) + bd_ref[layer : layer + 1].astype(f32) for layer in range(2)]
    b_row = bup_ref[0:1].astype(f32)
    q_cols = [column(q_ref, layer) for layer in range(2)]
    k_cols = [column(k_ref, layer) for layer in range(2)]
    items = images * chips
    ready = [due - 2 * number + 1 for due, due_events in events.items() for kind, number, _ in due_events if kind == "pair"]
    second = max([LEAD + items] + ready)

    def turn(index, carry):
        t = index - LEAD

        @pl.when(jnp.logical_and(t >= 0, t < 2 * items))
        def _():
            image = t // (2 * chips)
            step = lax.rem(t, 2 * chips) // 2
            sub = lax.rem(t, 2)
            span = pl.ds(pl.multiple_of(sub * quarter, quarter), quarter)
            for way in range(2):
                @pl.when(sub == 0)
                def _():
                    pair_arrival(image, way, step).wait_recv()

                local = from_partner[image, way, step, span].astype(f32) + mine[image, way, step, span].astype(f32)

                @pl.when(step == 0)
                def _():
                    ring[image, 0, way, sub] = local.astype(ring.dtype)

                @pl.when(step > 0)
                def _():
                    ring_copy(image, step - 1, way, sub).wait_recv()

                @pl.when(jnp.logical_and(step > 0, step < chips - 1))
                def _():
                    ring[image, step, way, sub] = (ring[image, step, way, sub].astype(f32) + local).astype(ring.dtype)

                @pl.when(step < chips - 1)
                def _():
                    ring_copy(image, step, way, sub).start()

                @pl.when(step == chips - 1)
                def _():
                    here = pl.ds(pl.multiple_of(image * seq_len + way * half + sub * quarter, quarter), quarter)
                    total = ring[image, chips - 1, way, sub].astype(f32) + local
                    middle = (own_x[here].astype(f32) + bias_rows[0] + total).astype(jnp.bfloat16).astype(f32)
                    h_ref[here] = norm_rows(middle, ln_rows[1])
                    acc_ref[here] = middle + bias_rows[1]

        for due, due_events in sorted(events.items()):
            @pl.when(index == due)
            def _():
                for event_args in due_events:
                    gather(*event_args)

        @pl.when(index < items)
        def _():
            @pl.when(index + 1 < items)
            def _():
                for copy in x_copies(index + 1):
                    copy.start()

            @pl.when(index >= 4)
            def _():
                for copy in pair_copies(index - 4):
                    copy.wait_send()

            for copy in x_copies(index):
                copy.wait()
            normed = norm_rows(x_buf[lax.rem(index, 2)].astype(f32), ln_rows[0])
            part = branches(normed, pack.at[0], b_row, q_cols[0], k_cols[0], seq_len, head_dim).astype(jnp.bfloat16)
            image, _, steps = place_of(index)
            for way in range(2):
                to_partner[lax.rem(index, 4), way] = part[way * half : (way + 1) * half]
                mine[image, way, steps[way]] = part[seq_len + way * half : seq_len + (way + 1) * half]
            for copy in pair_copies(index):
                copy.start()

        @pl.when(index == second - 1)
        def _():
            w_copy(0).start()

        @pl.when(index >= second)
        def _():
            m = index - second
            image = m // tp
            shard = lax.rem(m, tp)

            @pl.when(jnp.logical_and(image > 0, lax.rem(shard, 2) == 0))
            def _():
                event(image - 1, shard // 2)

            for number in range(chips):
                @pl.when(m == 2 * number)
                def _():
                    for copy in w_pair(number, 1 - core):
                        copy.wait_recv()

            @pl.when(m + 1 < images * tp)
            def _():
                w_copy(m + 1).start()

            w_copy(m).wait()
            slot = lax.rem(m, 2)
            span = pl.ds(pl.multiple_of(image * seq_len, seq_len), seq_len)
            owner = 2 * shard_of_round(chip, chips, shard // 2) + whose(shard)
            acc_ref[span] += branches(h_ref[span], w_buf.at[slot], b_all[owner][0:1], q_cols[1], k_cols[1], seq_len, head_dim)

            @pl.when(shard == tp - 1)
            def _():
                out_ref[pl.ds(pl.multiple_of(me * share + image * seq_len, seq_len), seq_len)] = acc_ref[span].astype(out_ref.dtype)
                for sub in range(2):
                    for way in range(2):
                        out_copy(image, way, sub, 0).start()
                for sub in range(2):
                    for way in range(2):
                        out_pair(image, way, sub, 0, core).start()

        return carry

    lax.fori_loop(0, second + images * tp, turn, 0)
    total = 2 * (chips - 1)
    done = tp // 2

    def tail(number, carry):
        @pl.when(number + done < total)
        def _():
            event(images - 2, number + done)

        event(images - 1, number)
        return carry

    lax.fori_loop(0, total, tail, 0)

    def drain(step, carry):
        for image in range(images):
            for way in range(2):
                for sub in range(2):
                    @pl.when(step < chips - 1)
                    def _():
                        ring_copy(image, step, way, sub).wait_send()
                        out_copy(image, way, sub, step).wait_send()

                    out_pair(image, way, sub, step, core).wait_send()
                    out_pair(image, way, sub, step, 1 - core).wait_recv()
        return carry

    lax.fori_loop(0, chips, drain, 0)
    for item in range(max(items - 4, 0), items):
        for copy in pair_copies(item):
            copy.wait_send()
    for number in range(chips):
        for copy in w_pair(number, core):
            copy.wait_send()
        for part in range(2 if number > 0 else 0):
            one, two = (plane[axis] for axis in axes(part))
            for hop in range(one - 1):
                line_copy(number, part, hop).wait_send()
            for hop in range(two - 1):
                for off in range(one):
                    plane_copy(number, part, off, hop).wait_send()
        if number > 0:
            for copy in z_copies(number):
                copy.wait_send()


def solution(mesh):
    col_spec = P(None, None, "tp")
    row_spec = P(None, "tp", None)
    in_specs = (P("dp", None, None), P(), col_spec, col_spec, col_spec, P(), P(), row_spec, P(), col_spec, P(None, "tp"), row_spec, P())
    tp = mesh.shape["tp"]
    dp = mesh.shape["dp"]
    chips = tp // 2

    def per_device(tokens_in, ln_scale, w_query, w_key, w_value, q_scale, k_scale, w_out, b_out, w_up, b_up, w_down, b_down):
        n_images, seq_len, model_dim = tokens_in.shape
        n_tokens = n_images * seq_len
        head_dim = q_scale.shape[1]
        mlp = w_up.shape[2]
        share = n_tokens // tp
        images = share // seq_len
        half, quarter = seq_len // 2, seq_len // 4
        rows = 4 * head_dim + 2 * mlp
        side = max(plane_of(dp))
        bf16, f32 = jnp.bfloat16, jnp.float32
        turned = [jnp.swapaxes(weight, 1, 2) for weight in (w_query, w_key, w_value)]
        hbm = pl.BlockSpec(memory_space=pltpu.HBM)
        vmem, dma = pltpu.VMEM, pltpu.SemaphoreType.DMA
        layers = ln_scale.shape[0]
        operands = (tokens_in.reshape(n_tokens, model_dim), *turned, w_up, w_down, w_out, ln_scale, b_out, b_down, b_up, q_scale, k_scale)
        out, _ = pl.pallas_call(
            functools.partial(layers_kernel, seq_len, head_dim, tp, dp),
            out_shape=(vmem((n_tokens, model_dim), bf16), jax.ShapeDtypeStruct((tp * rows, model_dim), bf16)),
            in_specs=[hbm] * 13,
            out_specs=(pl.BlockSpec(memory_space=pltpu.VMEM), hbm),
            scratch_shapes=[
                vmem((layers, model_dim), bf16), vmem((layers, model_dim), bf16), vmem((layers, model_dim), bf16), vmem((layers, mlp), bf16), vmem((layers, head_dim), bf16), vmem((layers, head_dim), bf16),
                vmem((layers, rows, model_dim), bf16), vmem((layers, model_dim, mlp), bf16),
                vmem((2, 2 * seq_len, model_dim), bf16), vmem((share, model_dim), bf16),
                vmem((images, chips, 2, 2, quarter, model_dim), bf16),
                vmem((images, 2, chips, half, model_dim), bf16), vmem((4, 2, half, model_dim), bf16), vmem((images, 2, chips, half, model_dim), bf16),
                vmem((tp, 8, mlp), f32), vmem((2, rows, model_dim), bf16), vmem((share, model_dim), bf16), vmem((share, model_dim), f32),
                dma((layers, 6)), dma((6,)), dma((2,)), dma((2, 2)),
                dma((images, chips, 2, 2)), dma((images, chips, 2, 2)), dma((images, 2, chips)), dma((images, 2, chips)),
                dma((chips, 2)), dma((chips, 2)), dma((chips,)), dma((chips,)),
                dma((chips, 2, side)), dma((chips, 2, side)), dma((chips, 2, side, side)), dma((chips, 2, side, side)),
                dma((chips,)), dma((chips,)), dma((chips,)), dma((chips,)), dma((2,)),
                dma((images, 2, 2, chips)), dma((images, 2, 2, chips)), dma((images, 2, 2, chips)), dma((images, 2, 2, chips)),
            ],
            compiler_params=pltpu.CompilerParams(vmem_limit_bytes=VMEM_BYTES, collective_id=0, has_side_effects=True),
            cost_estimate=pl.CostEstimate(flops=4 * n_tokens * model_dim * (rows + seq_len // 2), bytes_accessed=8 * n_tokens * model_dim, transcendentals=0),
            name="layers",
        )(*(pltpu.with_memory_space_constraint(value, pltpu.HBM) for value in operands))
        return out.reshape(n_images, seq_len, model_dim)

    return jax.shard_map(per_device, mesh=mesh, in_specs=in_specs, out_specs=P("dp", None, None), check_vma=False)
```

```python
import functools
import math

import jax
import jax.numpy as jnp
from jax import lax
from jax.experimental import pallas as pl
from jax.experimental.pallas import tpu as pltpu
from jax.sharding import PartitionSpec as P

LN_EPS = 1e-6
LOG2E = 1.4426950408889634
VMEM_BYTES = 45 * 1024 * 1024
LEAD = 3
COLUMNS = 256
NORM_ROWS = 16
WAIT = 2
MESH = pl.DeviceIdType.MESH


def norm_rows(values, scale_row):
    mean_val = jnp.mean(values, axis=-1, keepdims=True)
    centered = values - mean_val
    variance = jnp.mean(centered * centered, axis=-1, keepdims=True)
    return (centered * lax.rsqrt(variance + LN_EPS) * scale_row).astype(jnp.bfloat16)


def norm_cols(values, scale_col):
    mean_val = jnp.mean(values, axis=0, keepdims=True)
    centered = values - mean_val
    variance = jnp.mean(centered * centered, axis=0, keepdims=True)
    return (centered * lax.rsqrt(variance + LN_EPS) * scale_col).astype(jnp.bfloat16)


def branches(normed, w_ref, b_up, q_col, k_col, seq_len, head_dim, emit, between=None):
    tokens = normed.shape[0]
    mlp = b_up.shape[1]
    qkv = 3 * head_dim
    up_end = qkv + mlp
    proj = lax.dot_general(w_ref[0:qkv], normed, (((1,), (1,)), ((), ())), preferred_element_type=jnp.float32)
    queries = norm_cols(proj[0:head_dim], q_col)
    keys_all = norm_cols(proj[head_dim : 2 * head_dim], k_col)
    values_all = proj[2 * head_dim : qkv].astype(jnp.bfloat16)
    pre_act = lax.dot_general(normed, w_ref[qkv:up_end], (((1,), (1,)), ((), ())), preferred_element_type=jnp.float32)
    if between is not None:
        between()
    activated = jax.nn.gelu(pre_act + b_up, approximate=True).astype(jnp.bfloat16)
    mixed = []
    for img in range(tokens // seq_len):
        cols = slice(img * seq_len, (img + 1) * seq_len)
        scores = lax.dot_general(keys_all[:, cols], queries[:, cols], (((0,), (0,)), ((), ())), preferred_element_type=jnp.float32)
        top = jnp.max(scores, axis=0, keepdims=True)
        expd = jnp.exp2((scores - top) * (LOG2E * head_dim**-0.5))
        prob = (expd * (1.0 / jnp.sum(expd, axis=0, keepdims=True))).astype(jnp.bfloat16)
        mixed.append(jnp.dot(values_all[:, cols], prob, preferred_element_type=jnp.float32))
    mixed_rows = jnp.concatenate(mixed, axis=1).T.astype(jnp.bfloat16)
    both = jnp.concatenate([activated, mixed_rows], axis=1)
    for start in range(0, w_ref.shape[1], COLUMNS):
        cols = slice(start, min(start + COLUMNS, w_ref.shape[1]))
        emit(cols, jnp.dot(both, w_ref[up_end:, cols], preferred_element_type=jnp.float32))


def neighbours(tp):
    me = lax.axis_index("tp")
    chips = tp // 2
    core = lax.rem(me, 2)
    chip = me // 2
    right = lax.rem(chip + 1, chips) * 2 + core
    left = lax.rem(chip + chips - 1, chips) * 2 + core
    return core, chip, right, left, me + 1 - 2 * core


def enter(peers):
    barrier = pltpu.get_barrier_semaphore()
    for axis, peer in peers:
        pl.semaphore_signal(barrier, inc=1, device_id={axis: peer}, device_id_type=MESH)
    pl.semaphore_wait(barrier, len(peers))


def plane_of(dp):
    side = math.isqrt(dp)
    return (side, side) if side * side == dp else (1, dp)


def shard_of_round(chip, chips, number):
    sign = 1 - 2 * (number % 2)
    return lax.rem(chip + chips + sign * ((number + 1) // 2), chips)


def schedule_of(chips, plane):
    side = max(plane)
    events = {}
    for number in range(1, chips):
        begin = 4 + ((7 * (number - 1) + 1) // 2 if side < 3 else 3 * (number - 1))
        if number % 2 == 1:
            pair = (number + 1) // 2
            events.setdefault(begin, []).extend([("came", pair, 0), ("onward", pair, 0)])
            events.setdefault(begin + 2, []).append(("onward", pair, 1))
        events.setdefault(begin, []).append(("pass", number, 0))
        for hop in range(1, side):
            events.setdefault(begin + 1 + hop, []).append(("line", number, hop))
        for hop in range(1, side):
            events.setdefault(begin + 2 + side + hop, []).append(("plane", number, hop))
        events.setdefault(begin + 1 + 2 * side, []).append(("pair", number, 0))
    return events


def layers_kernel(
    seq_len, head_dim, tp, dp,
    x_hbm, wq_hbm, wk_hbm, wv_hbm, wup_hbm, wdown_hbm, wout_hbm, ln_hbm, bo_hbm, bd_hbm, bup_hbm, q_hbm, k_hbm,
    out_ref, w_all,
    ln_ref, bo_ref, bd_ref, bup_ref, q_ref, k_ref, pack, up_raw, x_buf, own_x, ring, from_partner, to_partner, mine, b_all, w_buf, h0_ref, h_ref, acc_ref,
    load_sem, small_sem, own_sem, x_sem, ring_send, ring_recv, pair_send, pair_recv, z_send, z_recv, zb_send, zb_recv,
    line_send, line_recv, plane_send, plane_recv, w_send, w_recv, wb_send, wb_recv, wl_sem, out_send, out_recv, outp_send, outp_recv,
):
    core, chip, right, left, partner = neighbours(tp)
    chips = tp // 2
    me = 2 * chip + core
    rows = pack.shape[1]
    mlp = up_raw.shape[2]
    qkv = 3 * head_dim
    share = own_x.shape[0]
    images = share // seq_len
    quarter = seq_len // 4
    half = seq_len // 2
    f32 = jnp.float32
    plane = plane_of(dp)
    group = lax.axis_index("dp")
    at = (group // plane[1], lax.rem(group, plane[1]))
    unit = rows // (2 * dp)

    def group_at(axis, pos, other):
        return pos * plane[1] + other if axis == 0 else other * plane[1] + pos

    def beside(axis, sign):
        return group_at(axis, lax.rem(at[axis] + plane[axis] + sign, plane[axis]), at[1 - axis])

    def loads(layer):
        pieces = [(wq_hbm, pack.at[layer, 0:head_dim]), (wk_hbm, pack.at[layer, head_dim : 2 * head_dim]), (wv_hbm, pack.at[layer, 2 * head_dim : qkv]), (wup_hbm, up_raw.at[layer]), (wdown_hbm, pack.at[layer, qkv + mlp : qkv + 2 * mlp]), (wout_hbm, pack.at[layer, qkv + 2 * mlp : rows])]
        return [pltpu.make_async_copy(src.at[layer], dst, load_sem.at[layer, place]) for place, (src, dst) in enumerate(pieces)]

    def turn_up(layer):
        for copy in loads(layer):
            copy.wait()
        pack[layer, qkv : qkv + mlp] = up_raw[layer].T

    small = [(ln_hbm, ln_ref), (bo_hbm, bo_ref), (bd_hbm, bd_ref), (bup_hbm, bup_ref), (q_hbm, q_ref), (k_hbm, k_ref)]
    small = [pltpu.make_async_copy(src, dst, small_sem.at[place]) for place, (src, dst) in enumerate(small)]

    def column(ref, layer):
        row = ref[layer : layer + 1].astype(f32)
        return jnp.broadcast_to(row, (8, head_dim)).T[:, 0:1]

    def block(number, start, count, owner):
        base = (2 * shard_of_round(chip, chips, number) + owner) * rows + start
        return w_all.at[pl.ds(pl.multiple_of(base, 8), count)]

    def z_copies(number):
        copies = []
        for part in range(2):
            rightwards = (part == 0) if number == chips - 1 else number % 2 == 1
            hops = (number + 1) // 2
            source = lax.rem(chip + chips + (1 - hops if rightwards else hops - 1), chips)
            peer = right if rightwards else left
            ref = w_all.at[pl.ds(pl.multiple_of((2 * source + core) * rows + (part * dp + group) * unit, 8), unit)]
            copies.append(pltpu.make_async_remote_copy(src_ref=ref, dst_ref=ref, send_sem=z_send.at[number, part], recv_sem=z_recv.at[number, part], device_id={"tp": peer}, device_id_type=MESH))
            if part == 0:
                ref = b_all.at[2 * source + core]
                copies.append(pltpu.make_async_remote_copy(src_ref=ref, dst_ref=ref, send_sem=zb_send.at[number], recv_sem=zb_recv.at[number], device_id={"tp": peer}, device_id_type=MESH))
        return copies

    def z_onward(number):
        if number == 0:
            return [(later, (0, 1)) for later in (1, 2) if later < chips - 1] or [(chips - 1, (0, 1))]
        if number + 2 < chips - 1:
            return [(number + 2, (0, 1))]
        if number < chips - 1:
            return [(chips - 1, (number % 2 == 0,))]
        return []

    def z_start(later, parts):
        copies = z_copies(later)
        for part in parts:
            if part == 0:
                copies[0].start()
                copies[1].start()
            else:
                copies[2].start()

    def axes(part):
        return (0, 1) if part == 0 else (1, 0)

    def sign_of(number):
        return 1 - 2 * (number % 2)

    def line_copy(number, part, hop):
        axis, sign = axes(part)[0], sign_of(number)
        source = group_at(axis, lax.rem(at[axis] + plane[axis] - sign * hop, plane[axis]), at[1 - axis])
        ref = block(number, (part * dp + source) * unit, unit, core)
        return pltpu.make_async_remote_copy(src_ref=ref, dst_ref=ref, send_sem=line_send.at[number, part, hop], recv_sem=line_recv.at[number, part, hop], device_id={"dp": beside(axis, sign)}, device_id_type=MESH)

    def plane_copy(number, part, off, hop):
        (one, two), sign = axes(part), sign_of(number)
        source = group_at(one, lax.rem(at[one] + plane[one] - sign * off, plane[one]), lax.rem(at[two] + plane[two] - sign * hop, plane[two]))
        ref = block(number, (part * dp + source) * unit, unit, core)
        return pltpu.make_async_remote_copy(src_ref=ref, dst_ref=ref, send_sem=plane_send.at[number, part, off, hop], recv_sem=plane_recv.at[number, part, off, hop], device_id={"dp": beside(two, sign)}, device_id_type=MESH)

    def w_pair(number, who):
        ref = block(number, 0, rows, who)
        bias = b_all.at[2 * shard_of_round(chip, chips, number) + who]
        return [
            pltpu.make_async_remote_copy(src_ref=ref, dst_ref=ref, send_sem=w_send.at[number], recv_sem=w_recv.at[number], device_id={"tp": partner}, device_id_type=MESH),
            pltpu.make_async_remote_copy(src_ref=bias, dst_ref=bias, send_sem=wb_send.at[number], recv_sem=wb_recv.at[number], device_id={"tp": partner}, device_id_type=MESH),
        ]

    def gather(kind, number, hop):
        both = [each for each in (2 * number - 1, 2 * number) if each < chips]
        if kind == "came":
            for each in both:
                for copy in z_copies(each):
                    copy.wait_recv()
        if kind == "onward":
            for each in both:
                for later, parts in z_onward(each):
                    if hop in parts:
                        z_start(later, (hop,))
        if kind == "pass":
            for part in range(2):
                if plane[axes(part)[0]] > 1:
                    line_copy(number, part, 0).start()
            for part in range(2):
                if plane[axes(part)[1]] > 1:
                    plane_copy(number, part, 0, 0).start()
        for part in range(2):
            one, two = (plane[axis] for axis in axes(part))
            if kind == "line" and hop < one:
                line_copy(number, part, hop - 1).wait_recv()
                if hop < one - 1:
                    line_copy(number, part, hop).start()
                if two > 1:
                    plane_copy(number, part, hop, 0).start()
            if kind == "plane" and hop < two:
                for off in range(one):
                    plane_copy(number, part, off, hop - 1).wait_recv()
                    if hop < two - 1:
                        plane_copy(number, part, off, hop).start()
        if kind == "pair":
            for copy in w_pair(number, core):
                copy.start()

    def place_of(item):
        image, number = item // chips, lax.rem(item, chips)
        near, odd, own = number // 2, lax.rem(number, 2), number // (chips - 1)
        far = chips - 2 - near
        there = lax.rem(chip + 2 * chips + (2 * odd - 1) * (1 + near) * (1 - own), chips)
        upper = (near * (1 - odd) + far * odd) * (1 - own) + (chips - 1) * own
        lower = (near * odd + far * (1 - odd)) * (1 - own) + (chips - 1) * own
        return image, there, (upper, lower)

    def x_copies(item):
        image, there, _ = place_of(item)
        slot = lax.rem(item, 2)
        return [
            pltpu.make_async_copy(
                x_hbm.at[pl.ds(pl.multiple_of((2 * there + owner) * share + image * seq_len, seq_len), seq_len)],
                x_buf.at[slot, pl.ds(place * seq_len, seq_len)],
                x_sem.at[slot, place],
            )
            for place, owner in ((0, 1 - core), (1, core))
        ]

    def pair_copies(item):
        image, _, steps = place_of(item)
        return [
            pltpu.make_async_remote_copy(
                src_ref=to_partner.at[lax.rem(item, 4), way], dst_ref=from_partner.at[image, way, steps[way]],
                send_sem=pair_send.at[image, way, steps[way]], recv_sem=pair_recv.at[image, way, steps[way]],
                device_id={"tp": partner}, device_id_type=MESH,
            )
            for way in range(2)
        ]

    def pair_arrival(image, way, step):
        return pltpu.make_async_remote_copy(
            src_ref=to_partner.at[0, way], dst_ref=from_partner.at[image, way, step],
            send_sem=pair_send.at[image, way, step], recv_sem=pair_recv.at[image, way, step],
            device_id={"tp": partner}, device_id_type=MESH,
        )

    def ring_copy(image, step, way, sub):
        return pltpu.make_async_remote_copy(
            src_ref=ring.at[image, step, way, sub], dst_ref=ring.at[image, step + 1, way, sub],
            send_sem=ring_send.at[image, step, way, sub], recv_sem=ring_recv.at[image, step, way, sub],
            device_id={"tp": left if way else right}, device_id_type=MESH,
        )

    def w_copy(turn):
        shard = lax.rem(turn, tp)
        slot = lax.rem(turn, 2)
        return pltpu.make_async_copy(block(shard // 2, 0, rows, whose(shard)), w_buf.at[slot], wl_sem.at[slot])

    def whose(shard):
        odd = lax.rem(shard, 2)
        return core + odd - 2 * core * odd

    def chunk(image, way, sub, owner):
        offset = owner * share + image * seq_len + way * (2 * quarter) + sub * quarter
        return out_ref.at[pl.ds(pl.multiple_of(offset, quarter), quarter)]

    def origin(way, step):
        back = chip - step if way == 0 else chip + step
        return 2 * lax.rem(back + chips, chips)

    def out_copy(image, way, sub, step):
        ref = chunk(image, way, sub, origin(way, step) + core)
        return pltpu.make_async_remote_copy(
            src_ref=ref, dst_ref=ref, send_sem=out_send.at[image, way, sub, step], recv_sem=out_recv.at[image, way, sub, step],
            device_id={"tp": left if way else right}, device_id_type=MESH,
        )

    def arrival(image, way, sub, step):
        ref = chunk(image, way, sub, origin(way, step + 1) + core)
        return pltpu.make_async_remote_copy(
            src_ref=ref, dst_ref=ref, send_sem=out_send.at[image, way, sub, step], recv_sem=out_recv.at[image, way, sub, step],
            device_id={"tp": left if way else right}, device_id_type=MESH,
        )

    def out_pair(image, way, sub, step, who):
        ref = chunk(image, way, sub, origin(way, step) + who)
        return pltpu.make_async_remote_copy(
            src_ref=ref, dst_ref=ref, send_sem=outp_send.at[image, way, sub, step], recv_sem=outp_recv.at[image, way, sub, step],
            device_id={"tp": partner}, device_id_type=MESH,
        )

    def event(image, number):
        step = number // 2
        sub = lax.rem(number, 2)
        for way in range(2):
            arrival(image, way, sub, step).wait_recv()

            @pl.when(step + 1 < chips - 1)
            def _():
                out_copy(image, way, sub, step + 1).start()

            out_pair(image, way, sub, step + 1, core).start()

    peers = [("tp", right), ("tp", left), ("tp", partner)]
    for axis in range(2):
        peers += [("dp", beside(axis, sign)) for sign in (1, -1)[: min(plane[axis] - 1, 2)]]
    enter(peers)

    for layer in (1, 0):
        for copy in loads(layer):
            copy.start()
        if layer == 1:
            for copy in small:
                copy.start()
    for item in range(2):
        for copy in x_copies(item):
            copy.start()
    own_load = pltpu.make_async_copy(x_hbm.at[pl.ds(pl.multiple_of(me * share, share), share)], own_x, own_sem.at[1])
    own_load.start()
    for copy in small:
        copy.wait()
    b_all[me] = jnp.broadcast_to(bup_ref[1:2].astype(f32), b_all.shape[1:])
    turn_up(1)
    own_copy = pltpu.make_async_copy(pack.at[1], w_all.at[pl.ds(pl.multiple_of(me * rows, 8), rows)], own_sem.at[0])
    own_copy.start()
    own_copy.wait()
    for later, parts in z_onward(0):
        z_start(later, parts)
    gather("pair", 0, 0)
    turn_up(0)
    own_load.wait()
    events = schedule_of(chips, plane)
    ln_rows = [ln_ref[layer : layer + 1].astype(f32) for layer in range(2)]
    bias_rows = [bo_ref[layer : layer + 1].astype(f32) + bd_ref[layer : layer + 1].astype(f32) for layer in range(2)]
    b_row = bup_ref[0:1].astype(f32)
    q_cols = [column(q_ref, layer) for layer in range(2)]
    k_cols = [column(k_ref, layer) for layer in range(2)]

    def norm_item(item):
        for start in range(0, 2 * seq_len, NORM_ROWS):
            here = slice(start, start + NORM_ROWS)
            h0_ref[here] = norm_rows(x_buf[lax.rem(item, 2), here].astype(f32), ln_rows[0])

    for copy in x_copies(0):
        copy.wait()
    norm_item(0)
    items = images * chips
    ready = [due - 2 * number + 1 for due, due_events in events.items() for kind, number, _ in due_events if kind == "pair"]
    second = max([LEAD + items] + ready)

    def turn(index, carry):
        t = index - LEAD

        @pl.when(jnp.logical_and(t >= 0, t < 2 * items))
        def _():
            image = t // (2 * chips)
            step = lax.rem(t, 2 * chips) // 2
            sub = lax.rem(t, 2)
            span = pl.ds(pl.multiple_of(sub * quarter, quarter), quarter)
            for way in range(2):
                @pl.when(sub == 0)
                def _():
                    pair_arrival(image, way, step).wait_recv()

                local = from_partner[image, way, step, span].astype(f32) + mine[image, way, step, span].astype(f32)

                @pl.when(step == 0)
                def _():
                    ring[image, 0, way, sub] = local.astype(ring.dtype)

                @pl.when(step > 0)
                def _():
                    ring_copy(image, step - 1, way, sub).wait_recv()

                @pl.when(jnp.logical_and(step > 0, step < chips - 1))
                def _():
                    ring[image, step, way, sub] = (ring[image, step, way, sub].astype(f32) + local).astype(ring.dtype)

                @pl.when(step < chips - 1)
                def _():
                    ring_copy(image, step, way, sub).start()

                @pl.when(step == chips - 1)
                def _():
                    here = pl.ds(pl.multiple_of(image * seq_len + way * half + sub * quarter, quarter), quarter)
                    total = ring[image, chips - 1, way, sub].astype(f32) + local
                    middle = (own_x[here].astype(f32) + bias_rows[0] + total).astype(jnp.bfloat16).astype(f32)
                    h_ref[here] = norm_rows(middle, ln_rows[1])
                    acc_ref[here] = middle + bias_rows[1]

        for due, due_events in sorted(events.items()):
            @pl.when(index == due)
            def _():
                for event_args in due_events:
                    gather(*event_args)

        @pl.when(index < items)
        def _():
            @pl.when(index + 1 < items)
            def _():
                for copy in x_copies(index + 1):
                    copy.wait()

            @pl.when(index + 2 < items)
            def _():
                for copy in x_copies(index + 2):
                    copy.start()

            @pl.when(index >= 4)
            def _():
                for copy in pair_copies(index - 4):
                    copy.wait_send()

            image, _, steps = place_of(index)

            def emit(cols, part):
                part = part.astype(jnp.bfloat16)
                for way in range(2):
                    to_partner[lax.rem(index, 4), way, :, cols] = part[way * half : (way + 1) * half]
                    mine[image, way, steps[way], :, cols] = part[seq_len + way * half : seq_len + (way + 1) * half]

            branches(h0_ref[...], pack.at[0], b_row, q_cols[0], k_cols[0], seq_len, head_dim, emit, lambda: norm_item(index + 1))
            for copy in pair_copies(index):
                copy.start()

        @pl.when(index == second - 1)
        def _():
            w_copy(0).start()

        @pl.when(index >= second)
        def _():
            m = index - second
            image = m // tp
            shard = lax.rem(m, tp)

            late = shard - WAIT

            @pl.when(jnp.logical_and(image > 0, jnp.logical_and(late >= 0, lax.rem(late, 4) < 3)))
            def _():
                event(image - 1, 3 * (late // 4) + lax.rem(late, 4))

            for number in range(chips):
                @pl.when(m == 2 * number)
                def _():
                    for copy in w_pair(number, 1 - core):
                        copy.wait_recv()

            @pl.when(m + 1 < images * tp)
            def _():
                w_copy(m + 1).start()

            w_copy(m).wait()
            slot = lax.rem(m, 2)
            span = pl.ds(pl.multiple_of(image * seq_len, seq_len), seq_len)
            owner = 2 * shard_of_round(chip, chips, shard // 2) + whose(shard)

            def emit(cols, part):
                acc_ref[span, cols] += part

            branches(h_ref[span], w_buf.at[slot], b_all[owner][0:1], q_cols[1], k_cols[1], seq_len, head_dim, emit)

            @pl.when(shard == tp - 1)
            def _():
                out_ref[pl.ds(pl.multiple_of(me * share + image * seq_len, seq_len), seq_len)] = acc_ref[span].astype(out_ref.dtype)
                for sub in range(2):
                    for way in range(2):
                        out_copy(image, way, sub, 0).start()
                for sub in range(2):
                    for way in range(2):
                        out_pair(image, way, sub, 0, core).start()

        return carry

    lax.fori_loop(0, second + images * tp, turn, 0)
    total = 2 * (chips - 1)
    done = sum(late % 4 < 3 for late in range(tp - WAIT))

    def tail(number, carry):
        @pl.when(number + done < total)
        def _():
            event(images - 2, number + done)

        event(images - 1, number)
        return carry

    lax.fori_loop(0, total, tail, 0)

    def drain(step, carry):
        for image in range(images):
            for way in range(2):
                for sub in range(2):
                    @pl.when(step < chips - 1)
                    def _():
                        ring_copy(image, step, way, sub).wait_send()
                        out_copy(image, way, sub, step).wait_send()

                    out_pair(image, way, sub, step, core).wait_send()
                    out_pair(image, way, sub, step, 1 - core).wait_recv()
        return carry

    lax.fori_loop(0, chips, drain, 0)
    for item in range(max(items - 4, 0), items):
        for copy in pair_copies(item):
            copy.wait_send()
    for number in range(chips):
        for copy in w_pair(number, core):
            copy.wait_send()
        for part in range(2 if number > 0 else 0):
            one, two = (plane[axis] for axis in axes(part))
            for hop in range(one - 1):
                line_copy(number, part, hop).wait_send()
            for hop in range(two - 1):
                for off in range(one):
                    plane_copy(number, part, off, hop).wait_send()
        if number > 0:
            for copy in z_copies(number):
                copy.wait_send()


def solution(mesh):
    col_spec = P(None, None, "tp")
    row_spec = P(None, "tp", None)
    in_specs = (P("dp", None, None), P(), col_spec, col_spec, col_spec, P(), P(), row_spec, P(), col_spec, P(None, "tp"), row_spec, P())
    tp = mesh.shape["tp"]
    dp = mesh.shape["dp"]
    chips = tp // 2

    def per_device(tokens_in, ln_scale, w_query, w_key, w_value, q_scale, k_scale, w_out, b_out, w_up, b_up, w_down, b_down):
        n_images, seq_len, model_dim = tokens_in.shape
        n_tokens = n_images * seq_len
        head_dim = q_scale.shape[1]
        mlp = w_up.shape[2]
        share = n_tokens // tp
        images = share // seq_len
        half, quarter = seq_len // 2, seq_len // 4
        rows = 4 * head_dim + 2 * mlp
        side = max(plane_of(dp))
        bf16, f32 = jnp.bfloat16, jnp.float32
        turned = [jnp.swapaxes(weight, 1, 2) for weight in (w_query, w_key, w_value)]
        hbm = pl.BlockSpec(memory_space=pltpu.HBM)
        vmem, dma = pltpu.VMEM, pltpu.SemaphoreType.DMA
        layers = ln_scale.shape[0]
        operands = (tokens_in.reshape(n_tokens, model_dim), *turned, w_up, w_down, w_out, ln_scale, b_out, b_down, b_up, q_scale, k_scale)
        out, _ = pl.pallas_call(
            functools.partial(layers_kernel, seq_len, head_dim, tp, dp),
            out_shape=(vmem((n_tokens, model_dim), bf16), jax.ShapeDtypeStruct((tp * rows, model_dim), bf16)),
            in_specs=[hbm] * 13,
            out_specs=(pl.BlockSpec(memory_space=pltpu.VMEM), hbm),
            scratch_shapes=[
                vmem((layers, model_dim), bf16), vmem((layers, model_dim), bf16), vmem((layers, model_dim), bf16), vmem((layers, mlp), bf16), vmem((layers, head_dim), bf16), vmem((layers, head_dim), bf16),
                vmem((layers, rows, model_dim), bf16), vmem((layers, model_dim, mlp), bf16),
                vmem((2, 2 * seq_len, model_dim), bf16), vmem((share, model_dim), bf16),
                vmem((images, chips, 2, 2, quarter, model_dim), bf16),
                vmem((images, 2, chips, half, model_dim), bf16), vmem((4, 2, half, model_dim), bf16), vmem((images, 2, chips, half, model_dim), bf16),
                vmem((tp, 8, mlp), f32), vmem((2, rows, model_dim), bf16), vmem((2 * seq_len, model_dim), bf16), vmem((share, model_dim), bf16), vmem((share, model_dim), f32),
                dma((layers, 6)), dma((6,)), dma((2,)), dma((2, 2)),
                dma((images, chips, 2, 2)), dma((images, chips, 2, 2)), dma((images, 2, chips)), dma((images, 2, chips)),
                dma((chips, 2)), dma((chips, 2)), dma((chips,)), dma((chips,)),
                dma((chips, 2, side)), dma((chips, 2, side)), dma((chips, 2, side, side)), dma((chips, 2, side, side)),
                dma((chips,)), dma((chips,)), dma((chips,)), dma((chips,)), dma((2,)),
                dma((images, 2, 2, chips)), dma((images, 2, 2, chips)), dma((images, 2, 2, chips)), dma((images, 2, 2, chips)),
            ],
            compiler_params=pltpu.CompilerParams(vmem_limit_bytes=VMEM_BYTES, collective_id=0, has_side_effects=True),
            cost_estimate=pl.CostEstimate(flops=4 * n_tokens * model_dim * (rows + seq_len // 2), bytes_accessed=8 * n_tokens * model_dim, transcendentals=0),
            name="layers",
        )(*(pltpu.with_memory_space_constraint(value, pltpu.HBM) for value in operands))
        return out.reshape(n_images, seq_len, model_dim)

    return jax.shard_map(per_device, mesh=mesh, in_specs=in_specs, out_specs=P("dp", None, None), check_vma=False)
```

```python
import functools
import math

import jax
import jax.numpy as jnp
from jax import lax
from jax.experimental import pallas as pl
from jax.experimental.pallas import tpu as pltpu
from jax.sharding import PartitionSpec as P

LN_EPS = 1e-6
LOG2E = 1.4426950408889634
VMEM_BYTES = 45 * 1024 * 1024
LEAD = 3
COLUMNS = 256
NORM_ROWS = 16
WAIT = 2
MESH = pl.DeviceIdType.MESH


def norm_rows(values, scale_row):
    mean_val = jnp.mean(values, axis=-1, keepdims=True)
    centered = values - mean_val
    variance = jnp.mean(centered * centered, axis=-1, keepdims=True)
    return (centered * lax.rsqrt(variance + LN_EPS) * scale_row).astype(jnp.bfloat16)


def norm_cols(values, scale_col):
    mean_val = jnp.mean(values, axis=0, keepdims=True)
    centered = values - mean_val
    variance = jnp.mean(centered * centered, axis=0, keepdims=True)
    return (centered * lax.rsqrt(variance + LN_EPS) * scale_col).astype(jnp.bfloat16)


def branches(normed, w_ref, b_up, q_col, k_col, seq_len, head_dim, emit, between=None):
    tokens = normed.shape[0]
    mlp = b_up.shape[1]
    qkv = 3 * head_dim
    up_end = qkv + mlp
    proj = lax.dot_general(w_ref[0:qkv], normed, (((1,), (1,)), ((), ())), preferred_element_type=jnp.float32)
    queries = norm_cols(proj[0:head_dim], q_col)
    keys_all = norm_cols(proj[head_dim : 2 * head_dim], k_col)
    values_all = proj[2 * head_dim : qkv].astype(jnp.bfloat16)
    pre_act = lax.dot_general(normed, w_ref[qkv:up_end], (((1,), (1,)), ((), ())), preferred_element_type=jnp.float32)
    if between is not None:
        between()
    activated = jax.nn.gelu(pre_act + b_up, approximate=True).astype(jnp.bfloat16)
    mixed = []
    for img in range(tokens // seq_len):
        cols = slice(img * seq_len, (img + 1) * seq_len)
        scores = lax.dot_general(keys_all[:, cols], queries[:, cols], (((0,), (0,)), ((), ())), preferred_element_type=jnp.float32)
        top = jnp.max(scores, axis=0, keepdims=True)
        expd = jnp.exp2((scores - top) * (LOG2E * head_dim**-0.5))
        prob = (expd * (1.0 / jnp.sum(expd, axis=0, keepdims=True))).astype(jnp.bfloat16)
        mixed.append(jnp.dot(values_all[:, cols], prob, preferred_element_type=jnp.float32))
    mixed_rows = jnp.concatenate(mixed, axis=1).T.astype(jnp.bfloat16)
    both = jnp.concatenate([activated, mixed_rows], axis=1)
    for start in range(0, w_ref.shape[1], COLUMNS):
        cols = slice(start, min(start + COLUMNS, w_ref.shape[1]))
        emit(cols, jnp.dot(both, w_ref[up_end:, cols], preferred_element_type=jnp.float32))


def neighbours(tp):
    me = lax.axis_index("tp")
    chips = tp // 2
    core = lax.rem(me, 2)
    chip = me // 2
    right = lax.rem(chip + 1, chips) * 2 + core
    left = lax.rem(chip + chips - 1, chips) * 2 + core
    return core, chip, right, left, me + 1 - 2 * core


def enter(peers):
    barrier = pltpu.get_barrier_semaphore()
    for axis, peer in peers:
        pl.semaphore_signal(barrier, inc=1, device_id={axis: peer}, device_id_type=MESH)
    pl.semaphore_wait(barrier, len(peers))


def plane_of(dp):
    side = math.isqrt(dp)
    return (side, side) if side * side == dp else (1, dp)


def shard_of_round(chip, chips, number):
    sign = 1 - 2 * (number % 2)
    return lax.rem(chip + chips + sign * ((number + 1) // 2), chips)


def schedule_of(chips, plane):
    side = max(plane)
    events = {}
    for number in range(1, chips):
        begin, lag = 4 + 3 * (number - 1), 0
        if side < 3 and number > 4:
            begin, lag = begin + 2 * (number - 5), 1
        if number % 2 == 1:
            pair = (number + 1) // 2
            events.setdefault(begin, []).extend([("came", pair, 0), ("onward", pair, 0)])
            events.setdefault(begin + 2, []).append(("onward", pair, 1))
        events.setdefault(begin, []).append(("pass", number, 0))
        for hop in range(1, side):
            events.setdefault(begin + lag + 1 + hop, []).append(("line", number, hop))
        for hop in range(1, side):
            events.setdefault(begin + lag + 2 + side + hop, []).append(("plane", number, hop))
        events.setdefault(begin + lag + 1 + 2 * side, []).append(("pair", number, 0))
    return events


def layers_kernel(
    seq_len, head_dim, tp, dp,
    x_hbm, wq_hbm, wk_hbm, wv_hbm, wup_hbm, wdown_hbm, wout_hbm, ln_hbm, bo_hbm, bd_hbm, bup_hbm, q_hbm, k_hbm,
    out_ref, w_all,
    ln_ref, bo_ref, bd_ref, bup_ref, q_ref, k_ref, pack, up_raw, x_buf, own_x, ring, from_partner, to_partner, mine, b_all, w_buf, h0_ref, h_ref, acc_ref,
    load_sem, small_sem, own_sem, x_sem, ring_send, ring_recv, pair_send, pair_recv, z_send, z_recv, zb_send, zb_recv,
    line_send, line_recv, plane_send, plane_recv, w_send, w_recv, wb_send, wb_recv, wl_sem, out_send, out_recv, outp_send, outp_recv,
):
    core, chip, right, left, partner = neighbours(tp)
    chips = tp // 2
    me = 2 * chip + core
    rows = pack.shape[1]
    mlp = up_raw.shape[2]
    qkv = 3 * head_dim
    share = own_x.shape[0]
    images = share // seq_len
    quarter = seq_len // 4
    half = seq_len // 2
    f32 = jnp.float32
    plane = plane_of(dp)
    group = lax.axis_index("dp")
    at = (group // plane[1], lax.rem(group, plane[1]))
    unit = rows // (2 * dp)

    def group_at(axis, pos, other):
        return pos * plane[1] + other if axis == 0 else other * plane[1] + pos

    def beside(axis, sign):
        return group_at(axis, lax.rem(at[axis] + plane[axis] + sign, plane[axis]), at[1 - axis])

    def loads(layer):
        pieces = [(wq_hbm, pack.at[layer, 0:head_dim]), (wk_hbm, pack.at[layer, head_dim : 2 * head_dim]), (wv_hbm, pack.at[layer, 2 * head_dim : qkv]), (wup_hbm, up_raw.at[layer]), (wdown_hbm, pack.at[layer, qkv + mlp : qkv + 2 * mlp]), (wout_hbm, pack.at[layer, qkv + 2 * mlp : rows])]
        return [pltpu.make_async_copy(src.at[layer], dst, load_sem.at[layer, place]) for place, (src, dst) in enumerate(pieces)]

    def turn_up(layer):
        for copy in loads(layer):
            copy.wait()
        pack[layer, qkv : qkv + mlp] = up_raw[layer].T

    small = [(ln_hbm, ln_ref), (bo_hbm, bo_ref), (bd_hbm, bd_ref), (bup_hbm, bup_ref), (q_hbm, q_ref), (k_hbm, k_ref)]
    small = [pltpu.make_async_copy(src, dst, small_sem.at[place]) for place, (src, dst) in enumerate(small)]

    def column(ref, layer):
        row = ref[layer : layer + 1].astype(f32)
        return jnp.broadcast_to(row, (8, head_dim)).T[:, 0:1]

    def block(number, start, count, owner):
        base = (2 * shard_of_round(chip, chips, number) + owner) * rows + start
        return w_all.at[pl.ds(pl.multiple_of(base, 8), count)]

    def z_copies(number):
        copies = []
        for part in range(2):
            rightwards = (part == 0) if number == chips - 1 else number % 2 == 1
            hops = (number + 1) // 2
            source = lax.rem(chip + chips + (1 - hops if rightwards else hops - 1), chips)
            peer = right if rightwards else left
            ref = w_all.at[pl.ds(pl.multiple_of((2 * source + core) * rows + (part * dp + group) * unit, 8), unit)]
            copies.append(pltpu.make_async_remote_copy(src_ref=ref, dst_ref=ref, send_sem=z_send.at[number, part], recv_sem=z_recv.at[number, part], device_id={"tp": peer}, device_id_type=MESH))
            if part == 0:
                ref = b_all.at[2 * source + core]
                copies.append(pltpu.make_async_remote_copy(src_ref=ref, dst_ref=ref, send_sem=zb_send.at[number], recv_sem=zb_recv.at[number], device_id={"tp": peer}, device_id_type=MESH))
        return copies

    def z_onward(number):
        if number == 0:
            return [(later, (0, 1)) for later in (1, 2) if later < chips - 1] or [(chips - 1, (0, 1))]
        if number + 2 < chips - 1:
            return [(number + 2, (0, 1))]
        if number < chips - 1:
            return [(chips - 1, (number % 2 == 0,))]
        return []

    def z_start(later, parts):
        copies = z_copies(later)
        for part in parts:
            if part == 0:
                copies[0].start()
                copies[1].start()
            else:
                copies[2].start()

    def axes(part):
        return (0, 1) if part == 0 else (1, 0)

    def sign_of(number):
        return 1 - 2 * (number % 2)

    def line_copy(number, part, hop):
        axis, sign = axes(part)[0], sign_of(number)
        source = group_at(axis, lax.rem(at[axis] + plane[axis] - sign * hop, plane[axis]), at[1 - axis])
        ref = block(number, (part * dp + source) * unit, unit, core)
        return pltpu.make_async_remote_copy(src_ref=ref, dst_ref=ref, send_sem=line_send.at[number, part, hop], recv_sem=line_recv.at[number, part, hop], device_id={"dp": beside(axis, sign)}, device_id_type=MESH)

    def plane_copy(number, part, off, hop):
        (one, two), sign = axes(part), sign_of(number)
        source = group_at(one, lax.rem(at[one] + plane[one] - sign * off, plane[one]), lax.rem(at[two] + plane[two] - sign * hop, plane[two]))
        ref = block(number, (part * dp + source) * unit, unit, core)
        return pltpu.make_async_remote_copy(src_ref=ref, dst_ref=ref, send_sem=plane_send.at[number, part, off, hop], recv_sem=plane_recv.at[number, part, off, hop], device_id={"dp": beside(two, sign)}, device_id_type=MESH)

    def w_pair(number, who):
        ref = block(number, 0, rows, who)
        bias = b_all.at[2 * shard_of_round(chip, chips, number) + who]
        return [
            pltpu.make_async_remote_copy(src_ref=ref, dst_ref=ref, send_sem=w_send.at[number], recv_sem=w_recv.at[number], device_id={"tp": partner}, device_id_type=MESH),
            pltpu.make_async_remote_copy(src_ref=bias, dst_ref=bias, send_sem=wb_send.at[number], recv_sem=wb_recv.at[number], device_id={"tp": partner}, device_id_type=MESH),
        ]

    def gather(kind, number, hop):
        both = [each for each in (2 * number - 1, 2 * number) if each < chips]
        if kind == "came":
            for each in both:
                for copy in z_copies(each):
                    copy.wait_recv()
        if kind == "onward":
            for each in both:
                for later, parts in z_onward(each):
                    if hop in parts:
                        z_start(later, (hop,))
        if kind == "pass":
            for part in range(2):
                if plane[axes(part)[0]] > 1:
                    line_copy(number, part, 0).start()
            for part in range(2):
                if plane[axes(part)[1]] > 1:
                    plane_copy(number, part, 0, 0).start()
        for part in range(2):
            one, two = (plane[axis] for axis in axes(part))
            if kind == "line" and hop < one:
                line_copy(number, part, hop - 1).wait_recv()
                if hop < one - 1:
                    line_copy(number, part, hop).start()
                if two > 1:
                    plane_copy(number, part, hop, 0).start()
            if kind == "plane" and hop < two:
                for off in range(one):
                    plane_copy(number, part, off, hop - 1).wait_recv()
                    if hop < two - 1:
                        plane_copy(number, part, off, hop).start()
        if kind == "pair":
            for copy in w_pair(number, core):
                copy.start()

    def place_of(item):
        image, number = item // chips, lax.rem(item, chips)
        near, odd, own = number // 2, lax.rem(number, 2), number // (chips - 1)
        far = chips - 2 - near
        there = lax.rem(chip + 2 * chips + (2 * odd - 1) * (1 + near) * (1 - own), chips)
        upper = (near * (1 - odd) + far * odd) * (1 - own) + (chips - 1) * own
        lower = (near * odd + far * (1 - odd)) * (1 - own) + (chips - 1) * own
        return image, there, (upper, lower)

    def x_copies(item):
        image, there, _ = place_of(item)
        slot = lax.rem(item, 2)
        return [
            pltpu.make_async_copy(
                x_hbm.at[pl.ds(pl.multiple_of((2 * there + owner) * share + image * seq_len, seq_len), seq_len)],
                x_buf.at[slot, pl.ds(place * seq_len, seq_len)],
                x_sem.at[slot, place],
            )
            for place, owner in ((0, 1 - core), (1, core))
        ]

    def pair_copies(item):
        image, _, steps = place_of(item)
        return [
            pltpu.make_async_remote_copy(
                src_ref=to_partner.at[lax.rem(item, 4), way], dst_ref=from_partner.at[image, way, steps[way]],
                send_sem=pair_send.at[image, way, steps[way]], recv_sem=pair_recv.at[image, way, steps[way]],
                device_id={"tp": partner}, device_id_type=MESH,
            )
            for way in range(2)
        ]

    def pair_arrival(image, way, step):
        return pltpu.make_async_remote_copy(
            src_ref=to_partner.at[0, way], dst_ref=from_partner.at[image, way, step],
            send_sem=pair_send.at[image, way, step], recv_sem=pair_recv.at[image, way, step],
            device_id={"tp": partner}, device_id_type=MESH,
        )

    def ring_copy(image, step, way, sub):
        return pltpu.make_async_remote_copy(
            src_ref=ring.at[image, step, way, sub], dst_ref=ring.at[image, step + 1, way, sub],
            send_sem=ring_send.at[image, step, way, sub], recv_sem=ring_recv.at[image, step, way, sub],
            device_id={"tp": left if way else right}, device_id_type=MESH,
        )

    def w_copy(turn):
        shard = lax.rem(turn, tp)
        slot = lax.rem(turn, 2)
        return pltpu.make_async_copy(block(shard // 2, 0, rows, whose(shard)), w_buf.at[slot], wl_sem.at[slot])

    def whose(shard):
        odd = lax.rem(shard, 2)
        return core + odd - 2 * core * odd

    def chunk(image, way, sub, owner):
        offset = owner * share + image * seq_len + way * (2 * quarter) + sub * quarter
        return out_ref.at[pl.ds(pl.multiple_of(offset, quarter), quarter)]

    def origin(way, step):
        back = chip - step if way == 0 else chip + step
        return 2 * lax.rem(back + chips, chips)

    def out_copy(image, way, sub, step):
        ref = chunk(image, way, sub, origin(way, step) + core)
        return pltpu.make_async_remote_copy(
            src_ref=ref, dst_ref=ref, send_sem=out_send.at[image, way, sub, step], recv_sem=out_recv.at[image, way, sub, step],
            device_id={"tp": left if way else right}, device_id_type=MESH,
        )

    def arrival(image, way, sub, step):
        ref = chunk(image, way, sub, origin(way, step + 1) + core)
        return pltpu.make_async_remote_copy(
            src_ref=ref, dst_ref=ref, send_sem=out_send.at[image, way, sub, step], recv_sem=out_recv.at[image, way, sub, step],
            device_id={"tp": left if way else right}, device_id_type=MESH,
        )

    def out_pair(image, way, sub, step, who):
        ref = chunk(image, way, sub, origin(way, step) + who)
        return pltpu.make_async_remote_copy(
            src_ref=ref, dst_ref=ref, send_sem=outp_send.at[image, way, sub, step], recv_sem=outp_recv.at[image, way, sub, step],
            device_id={"tp": partner}, device_id_type=MESH,
        )

    def event(image, number):
        step = number // 2
        sub = lax.rem(number, 2)
        for way in range(2):
            arrival(image, way, sub, step).wait_recv()

            @pl.when(step + 1 < chips - 1)
            def _():
                out_copy(image, way, sub, step + 1).start()

            out_pair(image, way, sub, step + 1, core).start()

    peers = [("tp", right), ("tp", left), ("tp", partner)]
    for axis in range(2):
        peers += [("dp", beside(axis, sign)) for sign in (1, -1)[: min(plane[axis] - 1, 2)]]
    enter(peers)

    for layer in (1, 0):
        for copy in loads(layer):
            copy.start()
        if layer == 1:
            for copy in small:
                copy.start()
    for item in range(2):
        for copy in x_copies(item):
            copy.start()
    own_load = pltpu.make_async_copy(x_hbm.at[pl.ds(pl.multiple_of(me * share, share), share)], own_x, own_sem.at[1])
    own_load.start()
    for copy in small:
        copy.wait()
    b_all[me] = jnp.broadcast_to(bup_ref[1:2].astype(f32), b_all.shape[1:])
    turn_up(1)
    own_copy = pltpu.make_async_copy(pack.at[1], w_all.at[pl.ds(pl.multiple_of(me * rows, 8), rows)], own_sem.at[0])
    own_copy.start()
    own_copy.wait()
    for later, parts in z_onward(0):
        z_start(later, parts)
    gather("pair", 0, 0)
    turn_up(0)
    own_load.wait()
    events = schedule_of(chips, plane)
    ln_rows = [ln_ref[layer : layer + 1].astype(f32) for layer in range(2)]
    bias_rows = [bo_ref[layer : layer + 1].astype(f32) + bd_ref[layer : layer + 1].astype(f32) for layer in range(2)]
    b_row = bup_ref[0:1].astype(f32)
    q_cols = [column(q_ref, layer) for layer in range(2)]
    k_cols = [column(k_ref, layer) for layer in range(2)]

    def norm_item(item):
        for start in range(0, 2 * seq_len, NORM_ROWS):
            here = slice(start, start + NORM_ROWS)
            h0_ref[here] = norm_rows(x_buf[lax.rem(item, 2), here].astype(f32), ln_rows[0])

    for copy in x_copies(0):
        copy.wait()
    norm_item(0)
    items = images * chips
    ready = [due - 2 * number + 1 for due, due_events in events.items() for kind, number, _ in due_events if kind == "pair"]
    second = max([LEAD + items] + ready)

    period = 2 * (chips - 1)

    def parts_of(image, step, way, sub):
        @pl.when(sub == 0)
        def _():
            pair_arrival(image, way, step).wait_recv()

        span = pl.ds(pl.multiple_of(sub * quarter, quarter), quarter)
        return from_partner[image, way, step, span].astype(f32) + mine[image, way, step, span].astype(f32)

    def turn(index, carry):
        t = index - LEAD

        @pl.when(jnp.logical_and(t >= 0, t < images * period))
        def _():
            image = t // period
            step = lax.rem(t, period) // 2
            sub = lax.rem(t, 2)
            for way in range(2):
                local = parts_of(image, step, way, sub)

                @pl.when(step == 0)
                def _():
                    ring[image, 0, way, sub] = local.astype(ring.dtype)

                @pl.when(step > 0)
                def _():
                    ring_copy(image, step - 1, way, sub).wait_recv()
                    ring[image, step, way, sub] = (ring[image, step, way, sub].astype(f32) + local).astype(ring.dtype)

                ring_copy(image, step, way, sub).start()

        @pl.when(jnp.logical_and(t >= period, jnp.logical_and(t < images * period + 2, lax.rem(t + period, period) < 2)))
        def _():
            image = t // period - 1
            sub = lax.rem(t, 2)
            for way in range(2):
                local = parts_of(image, chips - 1, way, sub)
                ring_copy(image, chips - 2, way, sub).wait_recv()
                here = pl.ds(pl.multiple_of(image * seq_len + way * half + sub * quarter, quarter), quarter)
                total = ring[image, chips - 1, way, sub].astype(f32) + local
                middle = (own_x[here].astype(f32) + bias_rows[0] + total).astype(jnp.bfloat16).astype(f32)
                h_ref[here] = norm_rows(middle, ln_rows[1])
                acc_ref[here] = middle + bias_rows[1]

        for due, due_events in sorted(events.items()):
            @pl.when(index == due)
            def _():
                for event_args in due_events:
                    gather(*event_args)

        @pl.when(index < items)
        def _():
            @pl.when(index + 1 < items)
            def _():
                for copy in x_copies(index + 1):
                    copy.wait()

            @pl.when(index + 2 < items)
            def _():
                for copy in x_copies(index + 2):
                    copy.start()

            @pl.when(index >= 4)
            def _():
                for copy in pair_copies(index - 4):
                    copy.wait_send()

            image, _, steps = place_of(index)

            def emit(cols, part):
                part = part.astype(jnp.bfloat16)
                for way in range(2):
                    to_partner[lax.rem(index, 4), way, :, cols] = part[way * half : (way + 1) * half]
                    mine[image, way, steps[way], :, cols] = part[seq_len + way * half : seq_len + (way + 1) * half]

            branches(h0_ref[...], pack.at[0], b_row, q_cols[0], k_cols[0], seq_len, head_dim, emit, lambda: norm_item(index + 1))
            for copy in pair_copies(index):
                copy.start()

        @pl.when(index == second - 1)
        def _():
            w_copy(0).start()

        @pl.when(index >= second)
        def _():
            m = index - second
            image = m // tp
            shard = lax.rem(m, tp)

            late = shard - WAIT

            @pl.when(jnp.logical_and(image > 0, jnp.logical_and(late >= 0, lax.rem(late, 4) < 3)))
            def _():
                event(image - 1, 3 * (late // 4) + lax.rem(late, 4))

            for number in range(chips):
                @pl.when(m == 2 * number)
                def _():
                    for copy in w_pair(number, 1 - core):
                        copy.wait_recv()

            @pl.when(m + 1 < images * tp)
            def _():
                w_copy(m + 1).start()

            w_copy(m).wait()
            slot = lax.rem(m, 2)
            span = pl.ds(pl.multiple_of(image * seq_len, seq_len), seq_len)
            owner = 2 * shard_of_round(chip, chips, shard // 2) + whose(shard)

            def emit(cols, part):
                acc_ref[span, cols] += part

            branches(h_ref[span], w_buf.at[slot], b_all[owner][0:1], q_cols[1], k_cols[1], seq_len, head_dim, emit)

            @pl.when(shard == tp - 1)
            def _():
                out_ref[pl.ds(pl.multiple_of(me * share + image * seq_len, seq_len), seq_len)] = acc_ref[span].astype(out_ref.dtype)
                for sub in range(2):
                    for way in range(2):
                        out_copy(image, way, sub, 0).start()
                for sub in range(2):
                    for way in range(2):
                        out_pair(image, way, sub, 0, core).start()

        return carry

    lax.fori_loop(0, second + images * tp, turn, 0)
    total = 2 * (chips - 1)
    done = sum(late % 4 < 3 for late in range(tp - WAIT))

    def tail(number, carry):
        @pl.when(number + done < total)
        def _():
            event(images - 2, number + done)

        event(images - 1, number)
        return carry

    lax.fori_loop(0, total, tail, 0)

    def drain(step, carry):
        for image in range(images):
            for way in range(2):
                for sub in range(2):
                    @pl.when(step < chips - 1)
                    def _():
                        ring_copy(image, step, way, sub).wait_send()
                        out_copy(image, way, sub, step).wait_send()

                    out_pair(image, way, sub, step, core).wait_send()
                    out_pair(image, way, sub, step, 1 - core).wait_recv()
        return carry

    lax.fori_loop(0, chips, drain, 0)
    for item in range(max(items - 4, 0), items):
        for copy in pair_copies(item):
            copy.wait_send()
    for number in range(chips):
        for copy in w_pair(number, core):
            copy.wait_send()
        for part in range(2 if number > 0 else 0):
            one, two = (plane[axis] for axis in axes(part))
            for hop in range(one - 1):
                line_copy(number, part, hop).wait_send()
            for hop in range(two - 1):
                for off in range(one):
                    plane_copy(number, part, off, hop).wait_send()
        if number > 0:
            for copy in z_copies(number):
                copy.wait_send()


def solution(mesh):
    col_spec = P(None, None, "tp")
    row_spec = P(None, "tp", None)
    in_specs = (P("dp", None, None), P(), col_spec, col_spec, col_spec, P(), P(), row_spec, P(), col_spec, P(None, "tp"), row_spec, P())
    tp = mesh.shape["tp"]
    dp = mesh.shape["dp"]
    chips = tp // 2

    def per_device(tokens_in, ln_scale, w_query, w_key, w_value, q_scale, k_scale, w_out, b_out, w_up, b_up, w_down, b_down):
        n_images, seq_len, model_dim = tokens_in.shape
        n_tokens = n_images * seq_len
        head_dim = q_scale.shape[1]
        mlp = w_up.shape[2]
        share = n_tokens // tp
        images = share // seq_len
        half, quarter = seq_len // 2, seq_len // 4
        rows = 4 * head_dim + 2 * mlp
        side = max(plane_of(dp))
        bf16, f32 = jnp.bfloat16, jnp.float32
        turned = [jnp.swapaxes(weight, 1, 2) for weight in (w_query, w_key, w_value)]
        hbm = pl.BlockSpec(memory_space=pltpu.HBM)
        vmem, dma = pltpu.VMEM, pltpu.SemaphoreType.DMA
        layers = ln_scale.shape[0]
        operands = (tokens_in.reshape(n_tokens, model_dim), *turned, w_up, w_down, w_out, ln_scale, b_out, b_down, b_up, q_scale, k_scale)
        out, _ = pl.pallas_call(
            functools.partial(layers_kernel, seq_len, head_dim, tp, dp),
            out_shape=(vmem((n_tokens, model_dim), bf16), jax.ShapeDtypeStruct((tp * rows, model_dim), bf16)),
            in_specs=[hbm] * 13,
            out_specs=(pl.BlockSpec(memory_space=pltpu.VMEM), hbm),
            scratch_shapes=[
                vmem((layers, model_dim), bf16), vmem((layers, model_dim), bf16), vmem((layers, model_dim), bf16), vmem((layers, mlp), bf16), vmem((layers, head_dim), bf16), vmem((layers, head_dim), bf16),
                vmem((layers, rows, model_dim), bf16), vmem((layers, model_dim, mlp), bf16),
                vmem((2, 2 * seq_len, model_dim), bf16), vmem((share, model_dim), bf16),
                vmem((images, chips, 2, 2, quarter, model_dim), bf16),
                vmem((images, 2, chips, half, model_dim), bf16), vmem((4, 2, half, model_dim), bf16), vmem((images, 2, chips, half, model_dim), bf16),
                vmem((tp, 8, mlp), f32), vmem((2, rows, model_dim), bf16), vmem((2 * seq_len, model_dim), bf16), vmem((share, model_dim), bf16), vmem((share, model_dim), f32),
                dma((layers, 6)), dma((6,)), dma((2,)), dma((2, 2)),
                dma((images, chips, 2, 2)), dma((images, chips, 2, 2)), dma((images, 2, chips)), dma((images, 2, chips)),
                dma((chips, 2)), dma((chips, 2)), dma((chips,)), dma((chips,)),
                dma((chips, 2, side)), dma((chips, 2, side)), dma((chips, 2, side, side)), dma((chips, 2, side, side)),
                dma((chips,)), dma((chips,)), dma((chips,)), dma((chips,)), dma((2,)),
                dma((images, 2, 2, chips)), dma((images, 2, 2, chips)), dma((images, 2, 2, chips)), dma((images, 2, 2, chips)),
            ],
            compiler_params=pltpu.CompilerParams(vmem_limit_bytes=VMEM_BYTES, collective_id=0, has_side_effects=True),
            cost_estimate=pl.CostEstimate(flops=4 * n_tokens * model_dim * (rows + seq_len // 2), bytes_accessed=8 * n_tokens * model_dim, transcendentals=0),
            name="layers",
        )(*(pltpu.with_memory_space_constraint(value, pltpu.HBM) for value in operands))
        return out.reshape(n_images, seq_len, model_dim)

    return jax.shard_map(per_device, mesh=mesh, in_specs=in_specs, out_specs=P("dp", None, None), check_vma=False)
```

```python
import functools
import math

import jax
import jax.numpy as jnp
from jax import lax
from jax.experimental import pallas as pl
from jax.experimental.pallas import tpu as pltpu
from jax.sharding import PartitionSpec as P

LN_EPS = 1e-6
LOG2E = 1.4426950408889634
VMEM_BYTES = 45 * 1024 * 1024
LEAD = 3
COLUMNS = 256
NORM_ROWS = 16
WAIT = 2
MESH = pl.DeviceIdType.MESH


def norm_rows(values, scale_row):
    mean_val = jnp.mean(values, axis=-1, keepdims=True)
    centered = values - mean_val
    variance = jnp.mean(centered * centered, axis=-1, keepdims=True)
    return (centered * lax.rsqrt(variance + LN_EPS) * scale_row).astype(jnp.bfloat16)


def norm_cols(values, scale_col):
    mean_val = jnp.mean(values, axis=0, keepdims=True)
    centered = values - mean_val
    variance = jnp.mean(centered * centered, axis=0, keepdims=True)
    return (centered * lax.rsqrt(variance + LN_EPS) * scale_col).astype(jnp.bfloat16)


def branches(normed, w_ref, b_up, q_col, k_col, seq_len, head_dim, emit, between=None):
    tokens = normed.shape[0]
    mlp = b_up.shape[1]
    qkv = 3 * head_dim
    up_end = qkv + mlp
    proj = lax.dot_general(w_ref[0:qkv], normed, (((1,), (1,)), ((), ())), preferred_element_type=jnp.float32)
    queries = norm_cols(proj[0:head_dim], q_col)
    keys_all = norm_cols(proj[head_dim : 2 * head_dim], k_col)
    values_all = proj[2 * head_dim : qkv].astype(jnp.bfloat16)
    pre_act = lax.dot_general(normed, w_ref[qkv:up_end], (((1,), (1,)), ((), ())), preferred_element_type=jnp.float32)
    if between is not None:
        between()
    activated = jax.nn.gelu(pre_act + b_up, approximate=True).astype(jnp.bfloat16)
    mixed = []
    for img in range(tokens // seq_len):
        cols = slice(img * seq_len, (img + 1) * seq_len)
        scores = lax.dot_general(keys_all[:, cols], queries[:, cols], (((0,), (0,)), ((), ())), preferred_element_type=jnp.float32)
        top = jnp.max(scores, axis=0, keepdims=True)
        expd = jnp.exp2((scores - top) * (LOG2E * head_dim**-0.5))
        prob = (expd * (1.0 / jnp.sum(expd, axis=0, keepdims=True))).astype(jnp.bfloat16)
        mixed.append(jnp.dot(values_all[:, cols], prob, preferred_element_type=jnp.float32))
    mixed_rows = jnp.concatenate(mixed, axis=1).T.astype(jnp.bfloat16)
    both = jnp.concatenate([activated, mixed_rows], axis=1)
    for start in range(0, w_ref.shape[1], COLUMNS):
        cols = slice(start, min(start + COLUMNS, w_ref.shape[1]))
        emit(cols, jnp.dot(both, w_ref[up_end:, cols], preferred_element_type=jnp.float32))


def neighbours(tp):
    me = lax.axis_index("tp")
    chips = tp // 2
    core = lax.rem(me, 2)
    chip = me // 2
    right = lax.rem(chip + 1, chips) * 2 + core
    left = lax.rem(chip + chips - 1, chips) * 2 + core
    return core, chip, right, left, me + 1 - 2 * core


def enter(peers):
    barrier = pltpu.get_barrier_semaphore()
    for axis, peer in peers:
        pl.semaphore_signal(barrier, inc=1, device_id={axis: peer}, device_id_type=MESH)
    pl.semaphore_wait(barrier, len(peers))


def plane_of(dp):
    side = math.isqrt(dp)
    return (side, side) if side * side == dp else (1, dp)


def shard_of_round(chip, chips, number):
    sign = 1 - 2 * (number % 2)
    return lax.rem(chip + chips + sign * ((number + 1) // 2), chips)


def schedule_of(chips, plane):
    side = max(plane)
    events = {}
    for number in range(1, chips):
        begin, lag = 4 + 3 * (number - 1), 0
        if side < 3 and number > 4:
            begin, lag = begin + 2 * (number - 5), 1
        if number % 2 == 1:
            pair = (number + 1) // 2
            events.setdefault(begin, []).extend([("came", pair, 0), ("onward", pair, 0)])
            events.setdefault(begin + 2, []).append(("onward", pair, 1))
        events.setdefault(begin, []).append(("pass", number, 0))
        for hop in range(1, side):
            events.setdefault(begin + lag + 1 + hop, []).append(("line", number, hop))
        for hop in range(1, side):
            events.setdefault(begin + lag + 2 + side + hop, []).append(("plane", number, hop))
        events.setdefault(begin + lag + 1 + 2 * side, []).append(("pair", number, 0))
    return events


def layers_kernel(
    seq_len, head_dim, tp, dp,
    x_hbm, wq_hbm, wk_hbm, wv_hbm, wup_hbm, wdown_hbm, wout_hbm, ln_hbm, bo_hbm, bd_hbm, bup_hbm, q_hbm, k_hbm,
    out_ref, w_all,
    ln_ref, bo_ref, bd_ref, bup_ref, q_ref, k_ref, pack, up_raw, x_buf, own_x, ring, from_partner, to_partner, mine, b_all, w_buf, h0_ref, h_ref, acc_ref,
    load_sem, small_sem, own_sem, x_sem, ring_send, ring_recv, pair_send, pair_recv, z_send, z_recv, zb_send, zb_recv,
    line_send, line_recv, plane_send, plane_recv, w_send, w_recv, wb_send, wb_recv, wl_sem, out_send, out_recv, outp_send, outp_recv,
):
    core, chip, right, left, partner = neighbours(tp)
    chips = tp // 2
    me = 2 * chip + core
    rows = pack.shape[1]
    mlp = up_raw.shape[2]
    qkv = 3 * head_dim
    share = own_x.shape[0]
    images = share // seq_len
    eighth = seq_len // 8
    half = seq_len // 2
    f32 = jnp.float32
    plane = plane_of(dp)
    group = lax.axis_index("dp")
    at = (group // plane[1], lax.rem(group, plane[1]))
    unit = rows // (2 * dp)

    def group_at(axis, pos, other):
        return pos * plane[1] + other if axis == 0 else other * plane[1] + pos

    def beside(axis, sign):
        return group_at(axis, lax.rem(at[axis] + plane[axis] + sign, plane[axis]), at[1 - axis])

    def loads(layer):
        pieces = [(wq_hbm, pack.at[layer, 0:head_dim]), (wk_hbm, pack.at[layer, head_dim : 2 * head_dim]), (wv_hbm, pack.at[layer, 2 * head_dim : qkv]), (wup_hbm, up_raw.at[layer]), (wdown_hbm, pack.at[layer, qkv + mlp : qkv + 2 * mlp]), (wout_hbm, pack.at[layer, qkv + 2 * mlp : rows])]
        return [pltpu.make_async_copy(src.at[layer], dst, load_sem.at[layer, place]) for place, (src, dst) in enumerate(pieces)]

    def turn_up(layer):
        for copy in loads(layer):
            copy.wait()
        pack[layer, qkv : qkv + mlp] = up_raw[layer].T

    small = [(ln_hbm, ln_ref), (bo_hbm, bo_ref), (bd_hbm, bd_ref), (bup_hbm, bup_ref), (q_hbm, q_ref), (k_hbm, k_ref)]
    small = [pltpu.make_async_copy(src, dst, small_sem.at[place]) for place, (src, dst) in enumerate(small)]

    def column(ref, layer):
        row = ref[layer : layer + 1].astype(f32)
        return jnp.broadcast_to(row, (8, head_dim)).T[:, 0:1]

    def block(number, start, count, owner):
        base = (2 * shard_of_round(chip, chips, number) + owner) * rows + start
        return w_all.at[pl.ds(pl.multiple_of(base, 8), count)]

    def z_copies(number):
        copies = []
        for part in range(2):
            rightwards = (part == 0) if number == chips - 1 else number % 2 == 1
            hops = (number + 1) // 2
            source = lax.rem(chip + chips + (1 - hops if rightwards else hops - 1), chips)
            peer = right if rightwards else left
            ref = w_all.at[pl.ds(pl.multiple_of((2 * source + core) * rows + (part * dp + group) * unit, 8), unit)]
            copies.append(pltpu.make_async_remote_copy(src_ref=ref, dst_ref=ref, send_sem=z_send.at[number, part], recv_sem=z_recv.at[number, part], device_id={"tp": peer}, device_id_type=MESH))
            if part == 0:
                ref = b_all.at[2 * source + core]
                copies.append(pltpu.make_async_remote_copy(src_ref=ref, dst_ref=ref, send_sem=zb_send.at[number], recv_sem=zb_recv.at[number], device_id={"tp": peer}, device_id_type=MESH))
        return copies

    def z_onward(number):
        if number == 0:
            return [(later, (0, 1)) for later in (1, 2) if later < chips - 1] or [(chips - 1, (0, 1))]
        if number + 2 < chips - 1:
            return [(number + 2, (0, 1))]
        if number < chips - 1:
            return [(chips - 1, (number % 2 == 0,))]
        return []

    def z_start(later, parts):
        copies = z_copies(later)
        for part in parts:
            if part == 0:
                copies[0].start()
                copies[1].start()
            else:
                copies[2].start()

    def axes(part):
        return (0, 1) if part == 0 else (1, 0)

    def sign_of(number):
        return 1 - 2 * (number % 2)

    def line_copy(number, part, hop):
        axis, sign = axes(part)[0], sign_of(number)
        source = group_at(axis, lax.rem(at[axis] + plane[axis] - sign * hop, plane[axis]), at[1 - axis])
        ref = block(number, (part * dp + source) * unit, unit, core)
        return pltpu.make_async_remote_copy(src_ref=ref, dst_ref=ref, send_sem=line_send.at[number, part, hop], recv_sem=line_recv.at[number, part, hop], device_id={"dp": beside(axis, sign)}, device_id_type=MESH)

    def plane_copy(number, part, off, hop):
        (one, two), sign = axes(part), sign_of(number)
        source = group_at(one, lax.rem(at[one] + plane[one] - sign * off, plane[one]), lax.rem(at[two] + plane[two] - sign * hop, plane[two]))
        ref = block(number, (part * dp + source) * unit, unit, core)
        return pltpu.make_async_remote_copy(src_ref=ref, dst_ref=ref, send_sem=plane_send.at[number, part, off, hop], recv_sem=plane_recv.at[number, part, off, hop], device_id={"dp": beside(two, sign)}, device_id_type=MESH)

    def w_pair(number, who):
        ref = block(number, 0, rows, who)
        bias = b_all.at[2 * shard_of_round(chip, chips, number) + who]
        return [
            pltpu.make_async_remote_copy(src_ref=ref, dst_ref=ref, send_sem=w_send.at[number], recv_sem=w_recv.at[number], device_id={"tp": partner}, device_id_type=MESH),
            pltpu.make_async_remote_copy(src_ref=bias, dst_ref=bias, send_sem=wb_send.at[number], recv_sem=wb_recv.at[number], device_id={"tp": partner}, device_id_type=MESH),
        ]

    def gather(kind, number, hop):
        both = [each for each in (2 * number - 1, 2 * number) if each < chips]
        if kind == "came":
            for each in both:
                for copy in z_copies(each):
                    copy.wait_recv()
        if kind == "onward":
            for each in both:
                for later, parts in z_onward(each):
                    if hop in parts:
                        z_start(later, (hop,))
        if kind == "pass":
            for part in range(2):
                if plane[axes(part)[0]] > 1:
                    line_copy(number, part, 0).start()
            for part in range(2):
                if plane[axes(part)[1]] > 1:
                    plane_copy(number, part, 0, 0).start()
        for part in range(2):
            one, two = (plane[axis] for axis in axes(part))
            if kind == "line" and hop < one:
                line_copy(number, part, hop - 1).wait_recv()
                if hop < one - 1:
                    line_copy(number, part, hop).start()
                if two > 1:
                    plane_copy(number, part, hop, 0).start()
            if kind == "plane" and hop < two:
                for off in range(one):
                    plane_copy(number, part, off, hop - 1).wait_recv()
                    if hop < two - 1:
                        plane_copy(number, part, off, hop).start()
        if kind == "pair":
            for copy in w_pair(number, core):
                copy.start()

    def place_of(item):
        image, number = item // chips, lax.rem(item, chips)
        near, odd, own = number // 2, lax.rem(number, 2), number // (chips - 1)
        far = chips - 2 - near
        there = lax.rem(chip + 2 * chips + (2 * odd - 1) * (1 + near) * (1 - own), chips)
        upper = (near * (1 - odd) + far * odd) * (1 - own) + (chips - 1) * own
        lower = (near * odd + far * (1 - odd)) * (1 - own) + (chips - 1) * own
        return image, there, (upper, lower)

    def x_copies(item):
        image, there, _ = place_of(item)
        slot = lax.rem(item, 2)
        return [
            pltpu.make_async_copy(
                x_hbm.at[pl.ds(pl.multiple_of((2 * there + owner) * share + image * seq_len, seq_len), seq_len)],
                x_buf.at[slot, pl.ds(place * seq_len, seq_len)],
                x_sem.at[slot, place],
            )
            for place, owner in ((0, 1 - core), (1, core))
        ]

    def pair_copies(item):
        image, _, steps = place_of(item)
        return [
            pltpu.make_async_remote_copy(
                src_ref=to_partner.at[lax.rem(item, 4), way], dst_ref=from_partner.at[image, way, steps[way]],
                send_sem=pair_send.at[image, way, steps[way]], recv_sem=pair_recv.at[image, way, steps[way]],
                device_id={"tp": partner}, device_id_type=MESH,
            )
            for way in range(2)
        ]

    def pair_arrival(image, way, step):
        return pltpu.make_async_remote_copy(
            src_ref=to_partner.at[0, way], dst_ref=from_partner.at[image, way, step],
            send_sem=pair_send.at[image, way, step], recv_sem=pair_recv.at[image, way, step],
            device_id={"tp": partner}, device_id_type=MESH,
        )

    def ring_copy(image, step, way, sub):
        return pltpu.make_async_remote_copy(
            src_ref=ring.at[image, step, way, sub], dst_ref=ring.at[image, step + 1, way, sub],
            send_sem=ring_send.at[image, step, way, sub], recv_sem=ring_recv.at[image, step, way, sub],
            device_id={"tp": left if way else right}, device_id_type=MESH,
        )

    def w_copy(turn):
        shard = lax.rem(turn, tp)
        slot = lax.rem(turn, 2)
        return pltpu.make_async_copy(block(shard // 2, 0, rows, whose(shard)), w_buf.at[slot], wl_sem.at[slot])

    def whose(shard):
        odd = lax.rem(shard, 2)
        return core + odd - 2 * core * odd

    def chunk(image, way, sub, owner):
        offset = owner * share + image * seq_len + way * half + sub * eighth
        return out_ref.at[pl.ds(pl.multiple_of(offset, eighth), eighth)]

    def origin(way, step):
        back = chip - step if way == 0 else chip + step
        return 2 * lax.rem(back + chips, chips)

    def out_copy(image, way, sub, step):
        ref = chunk(image, way, sub, origin(way, step) + core)
        return pltpu.make_async_remote_copy(
            src_ref=ref, dst_ref=ref, send_sem=out_send.at[image, way, sub, step], recv_sem=out_recv.at[image, way, sub, step],
            device_id={"tp": left if way else right}, device_id_type=MESH,
        )

    def arrival(image, way, sub, step):
        ref = chunk(image, way, sub, origin(way, step + 1) + core)
        return pltpu.make_async_remote_copy(
            src_ref=ref, dst_ref=ref, send_sem=out_send.at[image, way, sub, step], recv_sem=out_recv.at[image, way, sub, step],
            device_id={"tp": left if way else right}, device_id_type=MESH,
        )

    def out_pair(image, way, sub, step, who):
        ref = chunk(image, way, sub, origin(way, step) + who)
        return pltpu.make_async_remote_copy(
            src_ref=ref, dst_ref=ref, send_sem=outp_send.at[image, way, sub, step], recv_sem=outp_recv.at[image, way, sub, step],
            device_id={"tp": partner}, device_id_type=MESH,
        )

    def event(image, number):
        step = number // 2
        for fine in range(2):
            sub = 2 * lax.rem(number, 2) + fine
            for way in range(2):
                arrival(image, way, sub, step).wait_recv()

                @pl.when(step + 1 < chips - 1)
                def _():
                    out_copy(image, way, sub, step + 1).start()

                out_pair(image, way, sub, step + 1, core).start()

    peers = [("tp", right), ("tp", left), ("tp", partner)]
    for axis in range(2):
        peers += [("dp", beside(axis, sign)) for sign in (1, -1)[: min(plane[axis] - 1, 2)]]
    enter(peers)

    for layer in (1, 0):
        for copy in loads(layer):
            copy.start()
        if layer == 1:
            for copy in small:
                copy.start()
    for item in range(2):
        for copy in x_copies(item):
            copy.start()
    own_load = pltpu.make_async_copy(x_hbm.at[pl.ds(pl.multiple_of(me * share, share), share)], own_x, own_sem.at[1])
    own_load.start()
    for copy in small:
        copy.wait()
    b_all[me] = jnp.broadcast_to(bup_ref[1:2].astype(f32), b_all.shape[1:])
    turn_up(1)
    own_copy = pltpu.make_async_copy(pack.at[1], w_all.at[pl.ds(pl.multiple_of(me * rows, 8), rows)], own_sem.at[0])
    own_copy.start()
    own_copy.wait()
    for later, parts in z_onward(0):
        z_start(later, parts)
    gather("pair", 0, 0)
    turn_up(0)
    own_load.wait()
    events = schedule_of(chips, plane)
    ln_rows = [ln_ref[layer : layer + 1].astype(f32) for layer in range(2)]
    bias_rows = [bo_ref[layer : layer + 1].astype(f32) + bd_ref[layer : layer + 1].astype(f32) for layer in range(2)]
    b_row = bup_ref[0:1].astype(f32)
    q_cols = [column(q_ref, layer) for layer in range(2)]
    k_cols = [column(k_ref, layer) for layer in range(2)]

    def norm_item(item):
        for start in range(0, 2 * seq_len, NORM_ROWS):
            here = slice(start, start + NORM_ROWS)
            h0_ref[here] = norm_rows(x_buf[lax.rem(item, 2), here].astype(f32), ln_rows[0])

    for copy in x_copies(0):
        copy.wait()
    norm_item(0)
    items = images * chips
    ready = [due - 2 * number + 1 for due, due_events in events.items() for kind, number, _ in due_events if kind == "pair"]
    second = max([LEAD + items] + ready)

    period = 2 * (chips - 1)

    def parts_of(image, step, way, sub):
        @pl.when(sub == 0)
        def _():
            pair_arrival(image, way, step).wait_recv()

        span = pl.ds(pl.multiple_of(sub * eighth, eighth), eighth)
        return from_partner[image, way, step, span].astype(f32) + mine[image, way, step, span].astype(f32)

    def turn(index, carry):
        t = index - LEAD

        @pl.when(jnp.logical_and(t >= 0, t < images * period))
        def _():
            image = t // period
            step = lax.rem(t, period) // 2
            for fine in range(2):
                sub = 2 * lax.rem(t, 2) + fine
                for way in range(2):
                    local = parts_of(image, step, way, sub)

                    @pl.when(step == 0)
                    def _():
                        ring[image, 0, way, sub] = local.astype(ring.dtype)

                    @pl.when(step > 0)
                    def _():
                        ring_copy(image, step - 1, way, sub).wait_recv()
                        ring[image, step, way, sub] = (ring[image, step, way, sub].astype(f32) + local).astype(ring.dtype)

                    ring_copy(image, step, way, sub).start()

        @pl.when(jnp.logical_and(t >= period, jnp.logical_and(t < images * period + 2, lax.rem(t + period, period) < 2)))
        def _():
            image = t // period - 1
            for fine in range(2):
                sub = 2 * lax.rem(t, 2) + fine
                for way in range(2):
                    local = parts_of(image, chips - 1, way, sub)
                    ring_copy(image, chips - 2, way, sub).wait_recv()
                    here = pl.ds(pl.multiple_of(image * seq_len + way * half + sub * eighth, eighth), eighth)
                    total = ring[image, chips - 1, way, sub].astype(f32) + local
                    middle = (own_x[here].astype(f32) + bias_rows[0] + total).astype(jnp.bfloat16).astype(f32)
                    h_ref[here] = norm_rows(middle, ln_rows[1])
                    acc_ref[here] = middle + bias_rows[1]

        for due, due_events in sorted(events.items()):
            @pl.when(index == due)
            def _():
                for event_args in due_events:
                    gather(*event_args)

        @pl.when(index < items)
        def _():
            @pl.when(index + 1 < items)
            def _():
                for copy in x_copies(index + 1):
                    copy.wait()

            @pl.when(index + 2 < items)
            def _():
                for copy in x_copies(index + 2):
                    copy.start()

            @pl.when(index >= 4)
            def _():
                for copy in pair_copies(index - 4):
                    copy.wait_send()

            image, _, steps = place_of(index)

            def emit(cols, part):
                part = part.astype(jnp.bfloat16)
                for way in range(2):
                    to_partner[lax.rem(index, 4), way, :, cols] = part[way * half : (way + 1) * half]
                    mine[image, way, steps[way], :, cols] = part[seq_len + way * half : seq_len + (way + 1) * half]

            branches(h0_ref[...], pack.at[0], b_row, q_cols[0], k_cols[0], seq_len, head_dim, emit, lambda: norm_item(index + 1))
            for copy in pair_copies(index):
                copy.start()

        @pl.when(index == second - 1)
        def _():
            w_copy(0).start()

        @pl.when(index >= second)
        def _():
            m = index - second
            image = m // tp
            shard = lax.rem(m, tp)

            late = shard - WAIT

            @pl.when(jnp.logical_and(image > 0, jnp.logical_and(late >= 0, lax.rem(late, 4) < 3)))
            def _():
                event(image - 1, 3 * (late // 4) + lax.rem(late, 4))

            for number in range(chips):
                @pl.when(m == 2 * number)
                def _():
                    for copy in w_pair(number, 1 - core):
                        copy.wait_recv()

            @pl.when(m + 1 < images * tp)
            def _():
                w_copy(m + 1).start()

            w_copy(m).wait()
            slot = lax.rem(m, 2)
            span = pl.ds(pl.multiple_of(image * seq_len, seq_len), seq_len)
            owner = 2 * shard_of_round(chip, chips, shard // 2) + whose(shard)

            def emit(cols, part):
                acc_ref[span, cols] += part

            branches(h_ref[span], w_buf.at[slot], b_all[owner][0:1], q_cols[1], k_cols[1], seq_len, head_dim, emit)

            @pl.when(shard == tp - 1)
            def _():
                out_ref[pl.ds(pl.multiple_of(me * share + image * seq_len, seq_len), seq_len)] = acc_ref[span].astype(out_ref.dtype)
                for sub in range(4):
                    for way in range(2):
                        out_copy(image, way, sub, 0).start()
                for sub in range(4):
                    for way in range(2):
                        out_pair(image, way, sub, 0, core).start()

        return carry

    lax.fori_loop(0, second + images * tp, turn, 0)
    total = 2 * (chips - 1)
    done = sum(late % 4 < 3 for late in range(tp - WAIT))

    def tail(number, carry):
        @pl.when(number + done < total)
        def _():
            event(images - 2, number + done)

        event(images - 1, number)
        return carry

    lax.fori_loop(0, total, tail, 0)

    def drain(step, carry):
        for image in range(images):
            for way in range(2):
                for sub in range(4):
                    @pl.when(step < chips - 1)
                    def _():
                        ring_copy(image, step, way, sub).wait_send()
                        out_copy(image, way, sub, step).wait_send()

                    out_pair(image, way, sub, step, core).wait_send()
                    out_pair(image, way, sub, step, 1 - core).wait_recv()
        return carry

    lax.fori_loop(0, chips, drain, 0)
    for item in range(max(items - 4, 0), items):
        for copy in pair_copies(item):
            copy.wait_send()
    for number in range(chips):
        for copy in w_pair(number, core):
            copy.wait_send()
        for part in range(2 if number > 0 else 0):
            one, two = (plane[axis] for axis in axes(part))
            for hop in range(one - 1):
                line_copy(number, part, hop).wait_send()
            for hop in range(two - 1):
                for off in range(one):
                    plane_copy(number, part, off, hop).wait_send()
        if number > 0:
            for copy in z_copies(number):
                copy.wait_send()


def solution(mesh):
    col_spec = P(None, None, "tp")
    row_spec = P(None, "tp", None)
    in_specs = (P("dp", None, None), P(), col_spec, col_spec, col_spec, P(), P(), row_spec, P(), col_spec, P(None, "tp"), row_spec, P())
    tp = mesh.shape["tp"]
    dp = mesh.shape["dp"]
    chips = tp // 2

    def per_device(tokens_in, ln_scale, w_query, w_key, w_value, q_scale, k_scale, w_out, b_out, w_up, b_up, w_down, b_down):
        n_images, seq_len, model_dim = tokens_in.shape
        n_tokens = n_images * seq_len
        head_dim = q_scale.shape[1]
        mlp = w_up.shape[2]
        share = n_tokens // tp
        images = share // seq_len
        half, eighth = seq_len // 2, seq_len // 8
        rows = 4 * head_dim + 2 * mlp
        side = max(plane_of(dp))
        bf16, f32 = jnp.bfloat16, jnp.float32
        turned = [jnp.swapaxes(weight, 1, 2) for weight in (w_query, w_key, w_value)]
        hbm = pl.BlockSpec(memory_space=pltpu.HBM)
        vmem, dma = pltpu.VMEM, pltpu.SemaphoreType.DMA
        layers = ln_scale.shape[0]
        operands = (tokens_in.reshape(n_tokens, model_dim), *turned, w_up, w_down, w_out, ln_scale, b_out, b_down, b_up, q_scale, k_scale)
        out, _ = pl.pallas_call(
            functools.partial(layers_kernel, seq_len, head_dim, tp, dp),
            out_shape=(vmem((n_tokens, model_dim), bf16), jax.ShapeDtypeStruct((tp * rows, model_dim), bf16)),
            in_specs=[hbm] * 13,
            out_specs=(pl.BlockSpec(memory_space=pltpu.VMEM), hbm),
            scratch_shapes=[
                vmem((layers, model_dim), bf16), vmem((layers, model_dim), bf16), vmem((layers, model_dim), bf16), vmem((layers, mlp), bf16), vmem((layers, head_dim), bf16), vmem((layers, head_dim), bf16),
                vmem((layers, rows, model_dim), bf16), vmem((layers, model_dim, mlp), bf16),
                vmem((2, 2 * seq_len, model_dim), bf16), vmem((share, model_dim), bf16),
                vmem((images, chips, 2, 4, eighth, model_dim), bf16),
                vmem((images, 2, chips, half, model_dim), bf16), vmem((4, 2, half, model_dim), bf16), vmem((images, 2, chips, half, model_dim), bf16),
                vmem((tp, 8, mlp), f32), vmem((2, rows, model_dim), bf16), vmem((2 * seq_len, model_dim), bf16), vmem((share, model_dim), bf16), vmem((share, model_dim), f32),
                dma((layers, 6)), dma((6,)), dma((2,)), dma((2, 2)),
                dma((images, chips, 2, 4)), dma((images, chips, 2, 4)), dma((images, 2, chips)), dma((images, 2, chips)),
                dma((chips, 2)), dma((chips, 2)), dma((chips,)), dma((chips,)),
                dma((chips, 2, side)), dma((chips, 2, side)), dma((chips, 2, side, side)), dma((chips, 2, side, side)),
                dma((chips,)), dma((chips,)), dma((chips,)), dma((chips,)), dma((2,)),
                dma((images, 2, 4, chips)), dma((images, 2, 4, chips)), dma((images, 2, 4, chips)), dma((images, 2, 4, chips)),
            ],
            compiler_params=pltpu.CompilerParams(vmem_limit_bytes=VMEM_BYTES, collective_id=0, has_side_effects=True),
            cost_estimate=pl.CostEstimate(flops=4 * n_tokens * model_dim * (rows + seq_len // 2), bytes_accessed=8 * n_tokens * model_dim, transcendentals=0),
            name="layers",
        )(*(pltpu.with_memory_space_constraint(value, pltpu.HBM) for value in operands))
        return out.reshape(n_images, seq_len, model_dim)

    return jax.shard_map(per_device, mesh=mesh, in_specs=in_specs, out_specs=P("dp", None, None), check_vma=False)
```
